512 devices in a mesh: groups: 2 (over y), expert: 64 (over z, core), hidden: 4 (over x).
Axes of the slice: x: 4, y: 2, z: 32, core: 2. Of those that a mesh axis runs over, the one named last changes fastest.
The devices are a block of a 4x16x32 slice.
Arguments:
- tokens: bfloat16 [2048, 4096], P(('groups', 'expert')), parts along dimension 0, may hold values from -6 to 6
- expert_ids: int32 [2048, 8], P(('groups', 'expert')), parts along dimension 0, may hold values from 0 to 31, all different within a row; in each aligned block of 16 rows (0 to 15, 16 to 31, ...) at most 8 rows name the same one
- router_scores: float32 [2048, 8], P(('groups', 'expert')), parts along dimension 0, may hold values from 0.05 to 1
- gate_weight: bfloat16 [64, 4096, 512], P('expert', None, 'hidden'), may hold values from -0.09375 to 0.09375
- up_weight: bfloat16 [64, 4096, 512], P('expert', None, 'hidden'), may hold values from -0.09375 to 0.09375
- down_weight: bfloat16 [64, 512, 4096], P('expert', 'hidden'), may hold values from -0.1875 to 0.1875
Outputs:
- moe_out: bfloat16 [2048, 4096], P(('groups', 'expert'), 'hidden'), parts along dimension 0
The draws below stay inside these ranges and needn't reach their ends.
There are 2 independent parts, one for each index of `groups`. The reference program is written for one: setup_inputs(seed, part) draws one part's arguments, and reference() takes and returns one part's arrays. A program takes and returns all parts, laid end to end along the dimension named above; an argument that names none is the same for every part. Nothing has to cross between parts.
Inputs may be any that keep to these rules, and one draw needn't show every extreme that they name: `expert_ids`: each row names 8 different experts. In each aligned block of 16 rows no expert is named by more than 8 rows, a bound that some block reaches.
All inputs are finite; a program needn't handle non-finite values.
Results may differ from the reference program's by a relative error of at most 0.012.
Values may be sent and summed in bfloat16 or wider, within the bound.
No kernel may reach another device: no remote copies, remote signals or barrier semaphores. Data moves between devices by JAX's collectives and lax.ppermute only.
A program may use at most 64 MiB of HBM per device.

```python
import math
import jax
import jax.numpy as jnp
import numpy as np
from jax import lax

D = 4096
HID = 1024
SPAN = 2
TOK_DEV = 16
TOKENS = 1024
EXPERTS = 32
SLOTS = 64
TOPK = 8
HS = 512
PIECE = 128
CAP = 8
N_EXPERT = 64


def block_levels(stream_key, shape, pieces, smallest, top_value):
    gain, own = 1.0, jax.random.fold_in(stream_key, 6)
    for dim, shards_of in pieces:
        heights = jnp.exp(jax.random.uniform(jax.random.fold_in(own, dim), (shards_of,), jnp.float32, smallest / len(pieces), top_value / len(pieces)))
        gain = gain * jnp.repeat(heights, shape[dim] // shards_of).reshape([-1 if axis == dim else 1 for axis in range(len(shape))])
    return gain


def deal_out(key, own, number, rows, number_of, top, limit, lean):
    sequence = jax.random.permutation(key, number_of)
    packed, ordinary = shares(number_of, rows * top, limit, lean, True), shares(number_of, rows * top, limit, lean, False)
    places = jnp.arange(number_of)

    def named(tallies, offset_by):
        used = int((tallies > 0).sum())
        fixed = max(1, used // 4)
        moved = fixed + (places - fixed + offset_by * (used - fixed)) % max(1, number_of - fixed)
        return jnp.zeros((number_of,), jnp.int32).at[sequence[jnp.where(places < fixed, places, moved)]].set(jnp.asarray(tallies, jnp.int32))

    tallies = jnp.where(number % 4 == 0, named(packed, number // 4), named(ordinary, number - number // 4 - 1))
    mixed = jax.random.permutation(jax.random.fold_in(own, 3), number_of)
    giver, sink = mixed[0:number_of // 2 * 2:2], mixed[1:number_of // 2 * 2:2]
    margin = jnp.minimum(tallies[giver] - 1, limit - tallies[sink]) // 2
    margin = jnp.where((giver == sequence[0]) | (sink == sequence[0]) | (tallies[sink] == 0), 0, jnp.maximum(margin, 0))
    moved = jax.random.randint(jax.random.fold_in(own, 4), (number_of // 2,), 0, 1 << 20) % (margin + 1)
    tallies = tallies.at[giver].add(-moved).at[sink].add(moved)
    members = jnp.searchsorted(jnp.cumsum(tallies), jnp.arange(rows * top), side="right").astype(jnp.int32)
    listing = members.reshape(top, rows).T
    listing = listing[jax.random.permutation(jax.random.fold_in(own, 1), rows)]
    offset_by = jax.random.randint(jax.random.fold_in(own, 2), (rows, 1), 0, top)
    return jnp.take_along_axis(listing, (jnp.arange(top)[None, :] + offset_by) % top, axis=1)


def shares(amount, total, most, skew, full):
    portions = [(1 << 20) // math.isqrt(rank ** skew) + 1 for rank in range(1, amount + 1)]
    largest = most if full else min(most, max(-(-total // amount), total * portions[0] // sum(portions)))
    least = 1 if total - largest >= amount - 1 else 0
    holding, surplus = [largest] + [least] * (amount - 1), total - largest - least * (amount - 1)
    while surplus > 0:
        movable = [i for i in range(1, amount) if holding[i] < largest] or [i for i in range(1, amount) if holding[i] < most]
        whole, remaining = sum([portions[i] for i in movable]), surplus
        for i in movable:
            addition = min(most - holding[i], max(1, remaining * portions[i] // whole), surplus)
            holding[i] = holding[i] + addition
            surplus = surplus - addition
    return np.array(holding)


def normal_values(own_key, shape, deviation, most, split=(), kind=jnp.bfloat16):
    gain = block_levels(own_key, shape, split, -0.22, 0.18) if split else 1.0
    entries = jax.random.normal(own_key, shape, jnp.float32) * deviation * gain
    return jnp.minimum(jnp.maximum(entries, -most), most).astype(kind)


def setup_inputs(seed: int = 0, part: int = 0) -> dict:
    arg_keys = jax.random.split(jax.random.key(seed), 7)
    part_splits = jax.random.split(jax.random.fold_in(arg_keys[6], part), 7)
    tokens = normal_values(part_splits[0], (TOKENS, D), 1.0, 6.0, ((0, 64),))
    expert_ids_keys = jax.random.split(jax.random.fold_in(part_splits[1], 1), TOKENS // TOK_DEV)
    expert_ids_turns = jax.random.permutation(jax.random.fold_in(part_splits[1], 3), TOKENS // TOK_DEV)
    expert_ids = jax.vmap(lambda own, number: deal_out(jax.random.fold_in(part_splits[1], 2), own, number, TOK_DEV, EXPERTS, TOPK, CAP, 2))(expert_ids_keys, expert_ids_turns).reshape((TOKENS, TOPK))
    router_scores = jnp.clip(jnp.exp(math.log(1.0) - 2.9957323 * jax.random.uniform(part_splits[2], (TOKENS, TOPK), jnp.float32) ** block_levels(part_splits[2], (TOKENS, TOPK), ((0, 64),), -0.2, 0.2)), 0.05, 1.0)
    gate_weight = normal_values(arg_keys[3], (SLOTS, D, HS), D ** -0.5, 0.09375, ((0, 64), (2, 4)))
    up_weight = normal_values(arg_keys[4], (SLOTS, D, HS), D ** -0.5, 0.09375, ((0, 64), (2, 4)))
    down_weight = normal_values(arg_keys[5], (SLOTS, HS, D), HID ** -0.5, 0.1875, ((0, 64), (1, 4)))
    return dict(tokens=tokens, expert_ids=expert_ids, router_scores=router_scores, gate_weight=gate_weight, up_weight=up_weight, down_weight=down_weight)


def routed_weights(router_scores):
    return 2.5 * router_scores / jnp.sum(router_scores, axis=1, keepdims=True)


def positions(pair_ids, expert_count):
    onehot = (pair_ids[:, None] == jnp.arange(expert_count, dtype=jnp.int32)[None, :]).astype(jnp.int32)
    before = jnp.cumsum(onehot, axis=0) - onehot
    return jnp.sum(before * onehot, axis=1).astype(jnp.int32)


def reference(tokens, expert_ids, router_scores, gate_weight, up_weight, down_weight):
    blocks = N_EXPERT
    pair_count = TOK_DEV * TOPK
    pair_ids = expert_ids.reshape(blocks, pair_count).astype(jnp.int32)
    position = jax.vmap(lambda block_ids: positions(block_ids, EXPERTS))(pair_ids)
    slot_index = (pair_ids * CAP + position).astype(jnp.int32)
    local_token = (jnp.arange(pair_count, dtype=jnp.int32) // TOPK).astype(jnp.int32)
    owner_start = jnp.full((blocks, EXPERTS * CAP), TOK_DEV, jnp.int32)
    owner_row = jax.vmap(lambda start_row, slot_row: start_row.at[slot_row].set(local_token))(owner_start, slot_index)
    routed = routed_weights(router_scores).reshape(blocks, pair_count)
    slot_weight = jax.vmap(lambda slot_row, weight_row: jnp.zeros((EXPERTS * CAP,), jnp.float32).at[slot_row].set(weight_row))(slot_index, routed)
    padded = jnp.concatenate([tokens.reshape(blocks, TOK_DEV, D), jnp.zeros((blocks, 1, D), tokens.dtype)], axis=1)
    flat_rows = padded.reshape(blocks * (TOK_DEV + 1), D)
    block_base = (jnp.arange(blocks, dtype=jnp.int32) * (TOK_DEV + 1))[:, None]
    row_table = (block_base + owner_row).astype(jnp.int32).reshape(blocks, EXPERTS, CAP)
    weight_table = slot_weight.reshape(blocks, EXPERTS, CAP)
    gate_slots = gate_weight.reshape(EXPERTS, SPAN, D, HS)
    up_slots = up_weight.reshape(EXPERTS, SPAN, D, HS)
    down_pieces = down_weight.reshape(EXPERTS, HID // PIECE, PIECE, D)

    def one_expert(running, expert):
        row_index = row_table[:, expert, :].reshape(-1)
        weight_col = weight_table[:, expert, :].reshape(-1)
        row_data = flat_rows[row_index]
        gate_full = jnp.transpose(gate_slots[expert], (1, 0, 2)).reshape(D, HID)
        up_full = jnp.transpose(up_slots[expert], (1, 0, 2)).reshape(D, HID)
        gate_val = jnp.dot(row_data, gate_full, preferred_element_type=jnp.float32)
        up_val = jnp.dot(row_data, up_full, preferred_element_type=jnp.float32)
        activated = (jax.nn.silu(gate_val) * up_val).astype(jnp.bfloat16)
        split_act = activated.reshape(-1, HID // PIECE, PIECE).astype(jnp.float32)
        products = jnp.einsum('rgp,gpd->grd', split_act, down_pieces[expert].astype(jnp.float32))
        rounded = lax.optimization_barrier(products.astype(jnp.bfloat16))
        summed = jnp.sum(rounded.astype(jnp.float32), axis=0)
        running = running.at[row_index].add(weight_col[:, None] * summed)
        return running, None

    start = jnp.zeros((blocks * (TOK_DEV + 1), D), jnp.float32)
    total, unused = lax.scan(one_expert, start, jnp.arange(EXPERTS, dtype=jnp.int32))
    total = total.reshape(blocks, TOK_DEV + 1, D)[:, :TOK_DEV, :].reshape(TOKENS, D)
    return total.astype(jnp.bfloat16)
```

```python
import jax
import jax.numpy as jnp
from jax import lax
from jax.sharding import PartitionSpec as P

SPAN = 2


def body(tokens, expert_ids, router_scores, gate_weight, up_weight, down_weight):
    experts = lax.axis_size("expert") // SPAN
    rows = lax.all_gather(tokens, "expert", axis=0, tiled=True)
    routed = 2.5 * router_scores / jnp.sum(router_scores, axis=1, keepdims=True)
    named = expert_ids[:, :, None] == jnp.arange(experts, dtype=jnp.int32)[None, None, :]
    weight_table = jnp.sum(jnp.where(named, routed[:, :, None], 0.0), axis=1)
    weights_all = lax.all_gather(weight_table, "expert", axis=0, tiled=True)
    mine = lax.axis_index("expert") // SPAN
    weight_col = lax.dynamic_slice_in_dim(weights_all, mine, 1, 1)
    down = lax.all_to_all(down_weight[0], "hidden", split_axis=1, concat_axis=0, tiled=True)
    both = jnp.concatenate([gate_weight[0], up_weight[0]], axis=1)
    width = gate_weight.shape[2]
    val = jnp.dot(rows, both, preferred_element_type=jnp.float32)
    act = (jax.nn.silu(val[:, :width]) * val[:, width:]).astype(jnp.bfloat16)
    act_all = lax.all_gather(act, "hidden", axis=1, tiled=True)
    out = jnp.dot(act_all, down, preferred_element_type=jnp.float32)
    out = (out * weight_col).astype(jnp.bfloat16)
    return lax.psum_scatter(out, "expert", scatter_dimension=0, tiled=True)


def solution(mesh):
    return jax.shard_map(
        body,
        mesh=mesh,
        in_specs=(
            P(("groups", "expert"), None),
            P(("groups", "expert"), None),
            P(("groups", "expert"), None),
            P("expert", None, "hidden"),
            P("expert", None, "hidden"),
            P("expert", "hidden", None),
        ),
        out_specs=P(("groups", "expert"), "hidden"),
        check_vma=False,
    )
```

```python
import jax
import jax.numpy as jnp
from jax import lax
from jax.experimental import pallas as pl
from jax.experimental.pallas import tpu as pltpu
from jax.sharding import PartitionSpec as P


SPAN = 2
CAP = 8
F32 = jnp.float32
BF = jnp.bfloat16
VM = pltpu.MemorySpace.VMEM


def pack_kernel(x_ref, ids_ref, scores_ref, tok_ref, out_ref, weight_ref):
    top, count = ids_ref.shape
    experts, halves, cap, part = out_ref.shape
    pairs = experts * cap
    scores = scores_ref[...]
    routed = 2.5 * scores / jnp.sum(scores, axis=0, keepdims=True)
    row = lax.broadcasted_iota(jnp.int32, (pairs, count), 0)
    expert = row // cap
    member = jnp.zeros((pairs, count), F32)
    weight = jnp.zeros((pairs, count), F32)
    for k in range(top):
        hit = ids_ref[k : k + 1, :] == expert
        member = jnp.where(hit, 1.0, member)
        weight = jnp.where(hit, routed[k : k + 1, :], weight)
    earlier = lax.broadcasted_iota(jnp.int32, (count, count), 0) < lax.broadcasted_iota(
        jnp.int32, (count, count), 1
    )
    place = jnp.dot(
        member.astype(BF), jnp.where(earlier, 1.0, 0.0).astype(BF), preferred_element_type=F32
    )
    mine = (member > 0.5) & (place == (row - expert * cap).astype(F32))
    weight_ref[...] = jnp.where(mine, weight, 0.0)
    chosen = jnp.where(mine, 1.0, 0.0).astype(BF)
    for h in range(halves):
        col = pl.multiple_of(x_ref[0] * (halves * part) + h * part, part)
        rows = jnp.dot(chosen, tok_ref[:, pl.ds(col, part)], preferred_element_type=F32)
        for e in range(experts):
            out_ref[e, h] = rows[e * cap : (e + 1) * cap].astype(BF)


def pack(x, ids, scores, tokens, experts, part):
    count = tokens.shape[0]
    return pl.pallas_call(
        pack_kernel,
        out_shape=(
            jax.ShapeDtypeStruct((experts, SPAN, CAP, part), BF),
            jax.ShapeDtypeStruct((experts * CAP, count), F32),
        ),
        in_specs=[pl.BlockSpec(memory_space=pltpu.MemorySpace.SMEM)] + [pl.BlockSpec(memory_space=VM)] * 3,
        out_specs=[pl.BlockSpec(memory_space=VM)] * 2,
        compiler_params=pltpu.CompilerParams(vmem_limit_bytes=24 << 20),
        name="pack",
    )(x, ids, scores, tokens)


def act_kernel(at_ref, *refs):
    piece_refs, gate_ref, up_ref, out_ref = refs[:10], refs[10], refs[11], refs[12]
    part = piece_refs[0].shape[1]
    full = piece_refs[0].shape[0]
    half = full // 2

    def weights(i):
        rows = pl.ds(pl.multiple_of(at_ref[i] * part, part), part)
        return gate_ref[rows, :], up_ref[rows, :]

    def product(i, rows):
        gate, up = weights(i)
        return (
            jnp.dot(rows, gate, preferred_element_type=F32),
            jnp.dot(rows, up, preferred_element_type=F32),
        )

    for b in range(2):
        gate_val = up_val = None
        for core in range(2):
            own, left, right, far_top, far_low = piece_refs[core * 5 : core * 5 + 5]
            far = (far_top, far_low)[b]
            for d, rows in enumerate((own[b * half : (b + 1) * half], left[b * half : (b + 1) * half],
                                      right[b * half : (b + 1) * half], far[...])):
                g, u = product(core * 4 + d, rows)
                gate_val = g if gate_val is None else gate_val + g
                up_val = u if up_val is None else up_val + u
        out_ref[b * half : (b + 1) * half, :] = (gate_val / (1.0 + jnp.exp(-gate_val)) * up_val).astype(BF)


def act_of(at, pieces, gate, up):
    return pl.pallas_call(
        act_kernel,
        out_shape=jax.ShapeDtypeStruct((pieces[0].shape[0], gate.shape[1]), BF),
        in_specs=[pl.BlockSpec(memory_space=pltpu.MemorySpace.SMEM)] + [pl.BlockSpec(memory_space=VM)] * 12,
        out_specs=pl.BlockSpec(memory_space=VM),
        compiler_params=pltpu.CompilerParams(vmem_limit_bytes=24 << 20),
        name="act",
    )(at, *pieces, gate, up)


def down_kernel(at_ref, own_ref, other_ref, keep_ref, got_ref, out_ref):
    blocks, width, part = keep_ref.shape
    own = jnp.concatenate([own_ref[at_ref[i]] for i in range(blocks)], axis=1)
    other = jnp.concatenate([other_ref[at_ref[i]] for i in range(blocks)], axis=1)
    keep = keep_ref[...].reshape(blocks * width, part)
    got = got_ref[...].reshape(blocks * width, part)
    val = jnp.dot(own, keep, preferred_element_type=F32)
    val = val + jnp.dot(other, got, preferred_element_type=F32)
    out_ref[...] = val.astype(BF)


def down_of(at, own, other, keep, got):
    return pl.pallas_call(
        down_kernel,
        out_shape=jax.ShapeDtypeStruct((own.shape[1], keep.shape[2]), BF),
        in_specs=[pl.BlockSpec(memory_space=pltpu.MemorySpace.SMEM)] + [pl.BlockSpec(memory_space=VM)] * 4,
        out_specs=pl.BlockSpec(memory_space=VM),
        compiler_params=pltpu.CompilerParams(vmem_limit_bytes=24 << 20),
        name="down",
    )(at, own, other, keep, got)


def combine_kernel(back_ref, weight_ref, out_ref):
    experts, halves, _, part = back_ref.shape
    weight = weight_ref[...]
    high = weight.astype(BF)
    rest = weight - high.astype(F32)
    middle = rest.astype(BF)
    low = (rest - middle.astype(F32)).astype(BF)
    over_rows = (((0,), (0,)), ((), ()))
    for h in range(halves):
        rows = jnp.concatenate([back_ref[e, h].astype(F32) for e in range(experts)], axis=0).astype(BF)
        val = None
        for term in (low, middle, high):
            more = lax.dot_general(term, rows, over_rows, preferred_element_type=F32)
            val = more if val is None else val + more
        out_ref[:, h * part : (h + 1) * part] = val.astype(BF)


def combine(back, weight):
    return pl.pallas_call(
        combine_kernel,
        out_shape=jax.ShapeDtypeStruct((weight.shape[1], back.shape[1] * back.shape[3]), BF),
        in_specs=[pl.BlockSpec(memory_space=VM)] * 2,
        out_specs=pl.BlockSpec(memory_space=VM),
        compiler_params=pltpu.CompilerParams(vmem_limit_bytes=24 << 20),
        name="combine",
    )(back, weight)


def body(tokens, expert_ids, router_scores, gate_weight, up_weight, down_weight):
    model_width = tokens.shape[1]
    slots, columns = lax.axis_size("expert"), lax.axis_size("hidden")
    experts = slots // SPAN
    part = model_width // (columns * SPAN)
    x = lax.axis_index("hidden").astype(jnp.int32)
    core = (lax.axis_index("expert") % SPAN).astype(jnp.int32)
    swap = [(i, i ^ 1) for i in range(slots)]
    up_x = [(i, (i + 1) % columns) for i in range(columns)]
    down_x = [(i, (i - 1) % columns) for i in range(columns)]

    def swapped(v):
        return lax.ppermute(v, "expert", swap)

    down = down_weight[0]
    arrived = [lax.dynamic_slice_in_dim(down, x * SPAN * part, SPAN * part, 1)]
    for s in range(1, columns):
        share = lax.dynamic_slice_in_dim(down, (x + s) % columns * SPAN * part, SPAN * part, 1)
        arrived.append(lax.ppermute(share, "hidden", [(i, (i + s) % columns) for i in range(columns)]))
    outgoing, weight = pack(
        x.reshape(1), expert_ids.T, router_scores.T, tokens, experts, part
    )
    own = lax.all_to_all(
        outgoing.reshape(slots, CAP, part), "expert", split_axis=0, concat_axis=0, tiled=True
    ).reshape(slots * CAP, part)
    half = slots * CAP // 2
    left = lax.ppermute(own, "hidden", up_x)
    right = lax.ppermute(own, "hidden", down_x)
    far_top = lax.ppermute(left[:half], "hidden", up_x)
    far_low = lax.ppermute(right[half:], "hidden", down_x)
    mine = (own, left, right, far_top, far_low)
    pieces = mine + tuple(swapped(v) for v in mine)
    turns = jnp.array([0, columns - 1, 1, 2], jnp.int32)
    at = ((x + turns) % columns) * SPAN
    at = jnp.concatenate([at + core, at + 1 - core])
    spread = jnp.stack(arrived)
    down_keep = lax.dynamic_slice_in_dim(spread, core * part, part, 2)
    down_got = swapped(lax.dynamic_slice_in_dim(spread, (1 - core) * part, part, 2))
    source = (x - jnp.arange(columns, dtype=jnp.int32)) % columns
    act = act_of(at, pieces, gate_weight[0], up_weight[0])
    act_own = lax.all_gather(act, "hidden", axis=0, tiled=False)
    act_other = swapped(act_own)
    val = down_of(source, act_own, act_other, down_keep, down_got)
    back = lax.all_to_all(
        val.reshape(slots, CAP, part), "expert", split_axis=0, concat_axis=0, tiled=True
    )
    return combine(back.reshape(experts, SPAN, CAP, part), weight)


def solution(mesh):
    return jax.shard_map(
        body,
        mesh=mesh,
        in_specs=(
            P(("groups", "expert"), None),
            P(("groups", "expert"), None),
            P(("groups", "expert"), None),
            P("expert", None, "hidden"),
            P("expert", None, "hidden"),
            P("expert", "hidden", None),
        ),
        out_specs=P(("groups", "expert"), "hidden"),
        check_vma=False,
    )
```

```python
import jax
import jax.numpy as jnp
from jax import lax
from jax.experimental import pallas as pl
from jax.experimental.pallas import tpu as pltpu
from jax.sharding import PartitionSpec as P


SPAN = 2
CAP = 8
F32 = jnp.float32
BF = jnp.bfloat16
VM = pltpu.MemorySpace.VMEM


def pack_kernel(x_ref, ids_ref, scores_ref, tok_ref, out_ref, weight_ref):
    top, count = ids_ref.shape
    experts, cap, part = out_ref.shape
    pairs = experts * cap
    scores = scores_ref[...]
    routed = 2.5 * scores / jnp.sum(scores, axis=0, keepdims=True)
    row = lax.broadcasted_iota(jnp.int32, (pairs, count), 0)
    expert = row // cap
    member = jnp.zeros((pairs, count), F32)
    weight = jnp.zeros((pairs, count), F32)
    for k in range(top):
        hit = ids_ref[k : k + 1, :] == expert
        member = jnp.where(hit, 1.0, member)
        weight = jnp.where(hit, routed[k : k + 1, :], weight)
    earlier = lax.broadcasted_iota(jnp.int32, (count, count), 0) < lax.broadcasted_iota(
        jnp.int32, (count, count), 1
    )
    place = jnp.dot(
        member.astype(BF), jnp.where(earlier, 1.0, 0.0).astype(BF), preferred_element_type=F32
    )
    mine = (member > 0.5) & (place == (row - expert * cap).astype(F32))
    weight_ref[...] = jnp.where(mine, weight, 0.0)
    chosen = jnp.where(mine, 1.0, 0.0).astype(BF)
    col = pl.multiple_of(x_ref[0] * part, part)
    rows = jnp.dot(chosen, tok_ref[:, pl.ds(col, part)], preferred_element_type=F32)
    for e in range(experts):
        out_ref[e] = rows[e * cap : (e + 1) * cap].astype(BF)


def pack(x, ids, scores, tokens, experts, part):
    count = tokens.shape[0]
    return pl.pallas_call(
        pack_kernel,
        out_shape=(
            jax.ShapeDtypeStruct((experts, CAP, part), BF),
            jax.ShapeDtypeStruct((experts * CAP, count), F32),
        ),
        in_specs=[pl.BlockSpec(memory_space=pltpu.MemorySpace.SMEM)] + [pl.BlockSpec(memory_space=VM)] * 3,
        out_specs=[pl.BlockSpec(memory_space=VM)] * 2,
        compiler_params=pltpu.CompilerParams(vmem_limit_bytes=24 << 20),
        name="pack",
    )(x, ids, scores, tokens)


def act_kernel(at_ref, own_ref, left_ref, right_ref, top_ref, low_ref, gate_ref, up_ref, gate2_ref, up2_ref, out_ref):
    part = own_ref.shape[1]
    width = gate_ref.shape[1]
    far = jnp.concatenate([top_ref[...], low_ref[...]], axis=0)
    val = None
    for d, rows in enumerate((own_ref[...], left_ref[...], right_ref[...], far)):
        at = pl.ds(pl.multiple_of(at_ref[d] * part, part), part)
        weights = jnp.concatenate([r[at, :] for r in (gate_ref, up_ref, gate2_ref, up2_ref)], axis=1)
        more = jnp.dot(rows, weights, preferred_element_type=F32)
        val = more if val is None else val + more
    for i in range(SPAN):
        gate = val[:, 2 * i * width : (2 * i + 1) * width]
        up = val[:, (2 * i + 1) * width : (2 * i + 2) * width]
        out_ref[i] = (gate / (1.0 + jnp.exp(-gate)) * up).astype(BF)


def act_of(at, pieces, weights):
    return pl.pallas_call(
        act_kernel,
        out_shape=jax.ShapeDtypeStruct((SPAN, pieces[0].shape[0], weights[0].shape[1]), BF),
        in_specs=[pl.BlockSpec(memory_space=pltpu.MemorySpace.SMEM)] + [pl.BlockSpec(memory_space=VM)] * 9,
        out_specs=pl.BlockSpec(memory_space=VM),
        compiler_params=pltpu.CompilerParams(vmem_limit_bytes=24 << 20),
        name="act",
    )(at, *pieces, *weights)


def down_kernel(at_ref, act_ref, own_ref, other_ref, out_ref):
    blocks, width, part = own_ref.shape
    val = None
    for slot, weights_ref in enumerate((own_ref, other_ref)):
        rows = jnp.concatenate([act_ref[at_ref[i], slot] for i in range(blocks)], axis=1)
        more = jnp.dot(rows, weights_ref[...].reshape(blocks * width, part), preferred_element_type=F32)
        val = more if val is None else val + more
    out_ref[...] = val.astype(BF)


def down_of(at, act, own, other):
    return pl.pallas_call(
        down_kernel,
        out_shape=jax.ShapeDtypeStruct((act.shape[2], own.shape[2]), BF),
        in_specs=[pl.BlockSpec(memory_space=pltpu.MemorySpace.SMEM)] + [pl.BlockSpec(memory_space=VM)] * 3,
        out_specs=pl.BlockSpec(memory_space=VM),
        compiler_params=pltpu.CompilerParams(vmem_limit_bytes=24 << 20),
        name="down",
    )(at, act, own, other)


def combine_kernel(back_ref, weight_ref, out_ref):
    experts = back_ref.shape[0]
    weight = weight_ref[...]
    high = weight.astype(BF)
    rest = weight - high.astype(F32)
    middle = rest.astype(BF)
    low = (rest - middle.astype(F32)).astype(BF)
    over_rows = (((0,), (0,)), ((), ()))
    rows = jnp.concatenate([back_ref[e].astype(F32) for e in range(experts)], axis=0).astype(BF)
    val = None
    for term in (low, middle, high):
        more = lax.dot_general(term, rows, over_rows, preferred_element_type=F32)
        val = more if val is None else val + more
    out_ref[...] = val.astype(BF)


def combine(back, weight):
    return pl.pallas_call(
        combine_kernel,
        out_shape=jax.ShapeDtypeStruct((weight.shape[1], back.shape[2]), BF),
        in_specs=[pl.BlockSpec(memory_space=VM)] * 2,
        out_specs=pl.BlockSpec(memory_space=VM),
        compiler_params=pltpu.CompilerParams(vmem_limit_bytes=24 << 20),
        name="combine",
    )(back, weight)


def body(tokens, expert_ids, router_scores, gate_weight, up_weight, down_weight):
    slots, columns = lax.axis_size("expert"), lax.axis_size("hidden")
    experts = slots // SPAN
    part = tokens.shape[1] // columns
    x = lax.axis_index("hidden").astype(jnp.int32)
    same_core = [[SPAN * z + core for z in range(experts)] for core in range(SPAN)]
    swap = [(i, i ^ 1) for i in range(slots)]

    def turned(v, s):
        return lax.ppermute(v, "hidden", [(i, (i + s) % columns) for i in range(columns)])

    def swapped(v):
        return lax.ppermute(v, "expert", swap)

    def exchanged(v):
        return lax.all_to_all(
            v, "expert", split_axis=0, concat_axis=0, tiled=True, axis_index_groups=same_core
        )

    arrived = []
    for s in range(columns):
        share = lax.dynamic_slice_in_dim(down_weight[0], (x + s) % columns * part, part, 1)
        arrived.append(turned(share, s) if s else share)
    outgoing, weight = pack(x.reshape(1), expert_ids.T, router_scores.T, tokens, experts, part)
    own = exchanged(outgoing).reshape(experts * CAP, part)
    half = experts * CAP // 2
    left, right = turned(own, 1), turned(own, columns - 1)
    gate_other, up_other = swapped(gate_weight[0]), swapped(up_weight[0])
    far_top, far_low = turned(left[:half], 1), turned(right[half:], columns - 1)
    down = jnp.stack(arrived)
    down_other = swapped(down)
    at = (x + jnp.array([0, columns - 1, 1, 2], jnp.int32)) % columns
    act = act_of(
        at, (own, left, right, far_top, far_low), (gate_weight[0], up_weight[0], gate_other, up_other)
    )
    act_all = lax.all_gather(act, "hidden", axis=0, tiled=False)
    source = (x - jnp.arange(columns, dtype=jnp.int32)) % columns
    val = down_of(source, act_all, down, down_other)
    back = exchanged(val.reshape(experts, CAP, part))
    return combine(back, weight)


def solution(mesh):
    return jax.shard_map(
        body,
        mesh=mesh,
        in_specs=(
            P(("groups", "expert"), None),
            P(("groups", "expert"), None),
            P(("groups", "expert"), None),
            P("expert", None, "hidden"),
            P("expert", None, "hidden"),
            P("expert", "hidden", None),
        ),
        out_specs=P(("groups", "expert"), "hidden"),
        check_vma=False,
    )
```

```python
import jax
import jax.numpy as jnp
from jax import lax
from jax.experimental import pallas as pl
from jax.experimental.pallas import tpu as pltpu
from jax.sharding import PartitionSpec as P


SPAN = 2
CAP = 8
CHUNKS = 2
F32 = jnp.float32
BF = jnp.bfloat16
VM = pltpu.MemorySpace.VMEM


def params():
    return pltpu.CompilerParams(vmem_limit_bytes=24 << 20)


def specs(count):
    return [pl.BlockSpec(memory_space=VM)] * count


def pack_kernel(x_ref, ids_ref, scores_ref, tok_ref, *out_refs):
    top, count = ids_ref.shape
    experts, cap, part = out_refs[0].shape
    pairs, quad = experts * cap, cap // CHUNKS
    scores = scores_ref[...]
    routed = 2.5 * scores / jnp.sum(scores, axis=0, keepdims=True)
    row = lax.broadcasted_iota(jnp.int32, (pairs, count), 0)
    expert = row // cap
    member = jnp.zeros((pairs, count), F32)
    weight = jnp.zeros((pairs, count), F32)
    for k in range(top):
        hit = ids_ref[k : k + 1, :] == expert
        member = jnp.where(hit, 1.0, member)
        weight = jnp.where(hit, routed[k : k + 1, :], weight)
    earlier = lax.broadcasted_iota(jnp.int32, (count, count), 0) < lax.broadcasted_iota(
        jnp.int32, (count, count), 1
    )
    place = jnp.dot(
        member.astype(BF), jnp.where(earlier, 1.0, 0.0).astype(BF), preferred_element_type=F32
    )
    first = lax.broadcasted_iota(jnp.int32, (pairs, part), 0) % cap < quad
    tokens = [
        tok_ref[:, pl.ds(pl.multiple_of(x_ref[0] * (2 * part) + h * part, part), part)] for h in range(2)
    ]
    for q in range(CHUNKS):
        mine = (member > 0.5) & (place == (row % quad + q * quad).astype(F32))
        out_refs[CHUNKS + q][...] = jnp.where(mine, weight, 0.0)
        chosen = jnp.where(mine, 1.0, 0.0).astype(BF)
        low, high = (jnp.dot(chosen, t, preferred_element_type=F32) for t in tokens)
        rows = jnp.where(first, low, high)
        for e in range(experts):
            out_refs[q][e] = rows[e * cap : (e + 1) * cap].astype(BF)


def pack(x, ids, scores, tokens, experts, part):
    count = tokens.shape[0]
    return pl.pallas_call(
        pack_kernel,
        out_shape=[jax.ShapeDtypeStruct((experts, CAP, part), BF)] * CHUNKS
        + [jax.ShapeDtypeStruct((experts * CAP, count), F32)] * CHUNKS,
        in_specs=[pl.BlockSpec(memory_space=pltpu.MemorySpace.SMEM)] + specs(3),
        out_specs=specs(2 * CHUNKS),
        compiler_params=params(),
        name="pack",
    )(x, ids, scores, tokens)


def picker(rows, half, across):
    quad = CAP // CHUNKS
    shape = (2 * rows, rows) if across else (rows, 2 * rows)
    i = lax.broadcasted_iota(jnp.int32, shape, 1 if across else 0)
    j = lax.broadcasted_iota(jnp.int32, shape, 0 if across else 1)
    return jnp.where(j == i // quad * CAP + half * quad + i % quad, 1.0, 0.0).astype(BF)


def act_kernel(at_ref, own_ref, left_ref, right_ref, top_ref, low_ref, gate_ref, up_ref, gate2_ref, up2_ref, out_ref):
    part = own_ref.shape[1]
    width = gate_ref.shape[1]
    far = jnp.concatenate([top_ref[...], low_ref[...]], axis=0)
    pick = [picker(own_ref.shape[0] // 2, h, False) for h in range(2)]
    val = None
    for d, rows in enumerate((own_ref[...], left_ref[...], right_ref[...], far)):
        for h in range(2):
            at = pl.ds(pl.multiple_of(at_ref[d] * (2 * part) + h * part, part), part)
            weights = jnp.concatenate([r[at, :] for r in (gate_ref, up_ref, gate2_ref, up2_ref)], axis=1)
            compact = jnp.dot(pick[h], rows, preferred_element_type=F32).astype(BF)
            more = jnp.dot(compact, weights, preferred_element_type=F32)
            val = more if val is None else val + more
    for i in range(SPAN):
        gate = val[:, 2 * i * width : (2 * i + 1) * width]
        up = val[:, (2 * i + 1) * width : (2 * i + 2) * width]
        out_ref[i] = (gate / (1.0 + jnp.exp(-gate)) * up).astype(BF)


def act_of(at, pieces, weights):
    return pl.pallas_call(
        act_kernel,
        out_shape=jax.ShapeDtypeStruct((SPAN, pieces[0].shape[0] // 2, weights[0].shape[1]), BF),
        in_specs=[pl.BlockSpec(memory_space=pltpu.MemorySpace.SMEM)] + specs(9),
        out_specs=pl.BlockSpec(memory_space=VM),
        compiler_params=params(),
        name="act",
    )(at, *pieces, *weights)


def down_kernel(at_ref, act_ref, own_ref, other_ref, out_ref):
    blocks, width, part = own_ref.shape
    count, half = act_ref.shape[2], part // 2
    val = None
    for slot, weights_ref in enumerate((own_ref, other_ref)):
        rows = jnp.concatenate([act_ref[at_ref[i], slot] for i in range(blocks)], axis=1)
        more = jnp.dot(rows, weights_ref[...].reshape(blocks * width, part), preferred_element_type=F32)
        val = more if val is None else val + more
    val = val.astype(BF)
    out = jnp.dot(picker(count, 0, True), val[:, :half], preferred_element_type=F32)
    out = out + jnp.dot(picker(count, 1, True), val[:, half:], preferred_element_type=F32)
    out_ref[...] = out.astype(BF)


def down_of(at, act, own, other):
    return pl.pallas_call(
        down_kernel,
        out_shape=jax.ShapeDtypeStruct((2 * act.shape[2], own.shape[2] // 2), BF),
        in_specs=[pl.BlockSpec(memory_space=pltpu.MemorySpace.SMEM)] + specs(3),
        out_specs=pl.BlockSpec(memory_space=VM),
        compiler_params=params(),
        name="down",
    )(at, act, own, other)


def combine_kernel(*refs):
    back_refs, weight_refs, out_ref = refs[:CHUNKS], refs[CHUNKS : 2 * CHUNKS], refs[2 * CHUNKS]
    experts, cap, part = back_refs[0].shape
    quad = cap // CHUNKS
    over_rows = (((0,), (0,)), ((), ()))
    val = [None, None]
    for back_ref, weight_ref in zip(back_refs, weight_refs):
        rows = jnp.concatenate([back_ref[e].astype(F32) for e in range(experts)], axis=0).astype(BF)
        weight = weight_ref[...]
        first = lax.broadcasted_iota(jnp.int32, weight.shape, 0) % cap < quad
        for h in range(2):
            part_weight = jnp.where(first == (h == 0), weight, 0.0)
            high = part_weight.astype(BF)
            rest = part_weight - high.astype(F32)
            middle = rest.astype(BF)
            low = (rest - middle.astype(F32)).astype(BF)
            for term in (low, middle, high):
                more = lax.dot_general(term, rows, over_rows, preferred_element_type=F32)
                val[h] = more if val[h] is None else val[h] + more
    for h in range(2):
        out_ref[:, h * part : (h + 1) * part] = val[h].astype(BF)


def combine(backs, weights):
    return pl.pallas_call(
        combine_kernel,
        out_shape=jax.ShapeDtypeStruct((weights[0].shape[1], 2 * backs[0].shape[2]), BF),
        in_specs=specs(2 * CHUNKS),
        out_specs=pl.BlockSpec(memory_space=VM),
        compiler_params=params(),
        name="combine",
    )(*backs, *weights)


def body(tokens, expert_ids, router_scores, gate_weight, up_weight, down_weight):
    slots, columns = lax.axis_size("expert"), lax.axis_size("hidden")
    experts = slots // SPAN
    width = tokens.shape[1] // columns
    part = width // 2
    x = lax.axis_index("hidden").astype(jnp.int32)
    same_core = [[SPAN * z + core for z in range(experts)] for core in range(SPAN)]
    swap = [(i, i ^ 1) for i in range(slots)]

    def turned(v, s):
        return lax.ppermute(v, "hidden", [(i, (i + s) % columns) for i in range(columns)])

    def swapped(v):
        return lax.ppermute(v, "expert", swap)

    def exchanged(v):
        return lax.all_to_all(
            v, "expert", split_axis=0, concat_axis=0, tiled=True, axis_index_groups=same_core
        )

    packed = pack(x.reshape(1), expert_ids.T, router_scores.T, tokens, experts, part)
    outgoing, weights = packed[:CHUNKS], packed[CHUNKS:]
    arrived = []
    for s in range(columns):
        share = lax.dynamic_slice_in_dim(down_weight[0], (x + s) % columns * width, width, 1)
        arrived.append(turned(share, s) if s else share)
    gate_other, up_other = swapped(gate_weight[0]), swapped(up_weight[0])
    down = jnp.stack(arrived)
    down_other = swapped(down)
    at = (x + jnp.array([0, columns - 1, 1, 2], jnp.int32)) % columns
    source = (x - jnp.arange(columns, dtype=jnp.int32)) % columns
    mine = []
    for q in range(CHUNKS):
        mine.append(exchanged(outgoing[q]).reshape(experts * CAP, part))
    half = experts * CAP // 2
    backs = []
    for q in range(CHUNKS):
        own = mine[q]
        left, right = turned(own, 1), turned(own, columns - 1)
        far_top, far_low = turned(left[:half], 1), turned(right[half:], columns - 1)
        act = act_of(
            at, (own, left, right, far_top, far_low), (gate_weight[0], up_weight[0], gate_other, up_other)
        )
        act_all = lax.all_gather(act, "hidden", axis=0, tiled=False)
        val = down_of(source, act_all, down, down_other)
        backs.append(exchanged(val.reshape(experts, CAP, part)))
    return combine(backs, weights)


def solution(mesh):
    return jax.shard_map(
        body,
        mesh=mesh,
        in_specs=(
            P(("groups", "expert"), None),
            P(("groups", "expert"), None),
            P(("groups", "expert"), None),
            P("expert", None, "hidden"),
            P("expert", None, "hidden"),
            P("expert", "hidden", None),
        ),
        out_specs=P(("groups", "expert"), "hidden"),
        check_vma=False,
    )
```

```python
import jax
import jax.numpy as jnp
from jax import lax
from jax.experimental import pallas as pl
from jax.experimental.pallas import tpu as pltpu
from jax.sharding import PartitionSpec as P


SPAN = 2
CAP = 8
F32 = jnp.float32
BF = jnp.bfloat16
VM = pltpu.MemorySpace.VMEM


def pack_kernel(x_ref, ids_ref, scores_ref, tok_ref, out_ref, weight_ref):
    top, count = ids_ref.shape
    experts, cap, part = out_ref.shape
    pairs = experts * cap
    scores = scores_ref[...]
    routed = 2.5 * scores / jnp.sum(scores, axis=0, keepdims=True)
    row = lax.broadcasted_iota(jnp.int32, (pairs, count), 0)
    expert = row // cap
    member = jnp.zeros((pairs, count), F32)
    weight = jnp.zeros((pairs, count), F32)
    for k in range(top):
        hit = ids_ref[k : k + 1, :] == expert
        member = jnp.where(hit, 1.0, member)
        weight = jnp.where(hit, routed[k : k + 1, :], weight)
    earlier = lax.broadcasted_iota(jnp.int32, (count, count), 0) < lax.broadcasted_iota(
        jnp.int32, (count, count), 1
    )
    place = jnp.dot(
        member.astype(BF), jnp.where(earlier, 1.0, 0.0).astype(BF), preferred_element_type=F32
    )
    mine = (member > 0.5) & (place == (row - expert * cap).astype(F32))
    weight_ref[...] = jnp.where(mine, weight, 0.0)
    chosen = jnp.where(mine, 1.0, 0.0).astype(BF)
    col = pl.multiple_of(x_ref[0] * part, part)
    rows = jnp.dot(chosen, tok_ref[:, pl.ds(col, part)], preferred_element_type=F32)
    for e in range(experts):
        out_ref[e] = rows[e * cap : (e + 1) * cap].astype(BF)


def pack(x, ids, scores, tokens, experts, part):
    count = tokens.shape[0]
    return pl.pallas_call(
        pack_kernel,
        out_shape=(
            jax.ShapeDtypeStruct((experts, CAP, part), BF),
            jax.ShapeDtypeStruct((experts * CAP, count), F32),
        ),
        in_specs=[pl.BlockSpec(memory_space=pltpu.MemorySpace.SMEM)] + [pl.BlockSpec(memory_space=VM)] * 3,
        out_specs=[pl.BlockSpec(memory_space=VM)] * 2,
        compiler_params=pltpu.CompilerParams(vmem_limit_bytes=24 << 20),
        name="pack",
    )(x, ids, scores, tokens)


def partial_kernel(at_ref, rows_ref, own_ref, other_ref, out_ref):
    rows = rows_ref[...]
    for s in range(own_ref.shape[0]):
        weights = jnp.concatenate([r[s, i] for r in (own_ref, other_ref) for i in range(2)], axis=1)
        out_ref[at_ref[s]] = jnp.dot(rows, weights, preferred_element_type=F32).astype(BF)


def partial_of(at, rows, own, other):
    blocks, _, _, width = own.shape
    return pl.pallas_call(
        partial_kernel,
        out_shape=jax.ShapeDtypeStruct((blocks, rows.shape[0], 2 * SPAN * width), BF),
        in_specs=[pl.BlockSpec(memory_space=pltpu.MemorySpace.SMEM)] + [pl.BlockSpec(memory_space=VM)] * 3,
        out_specs=pl.BlockSpec(memory_space=VM),
        compiler_params=pltpu.CompilerParams(vmem_limit_bytes=24 << 20),
        name="partial",
    )(at, rows, own, other)


def act_kernel(parts_ref, out_ref):
    blocks = parts_ref.shape[0]
    width = out_ref.shape[3]
    val = parts_ref[0].astype(F32)
    for i in range(1, blocks):
        val = val + parts_ref[i].astype(F32)
    for i in range(SPAN):
        gate = val[:, 2 * i * width : (2 * i + 1) * width]
        up = val[:, (2 * i + 1) * width : (2 * i + 2) * width]
        act = (gate / (1.0 + jnp.exp(-gate)) * up).astype(BF)
        for copy in range(blocks):
            out_ref[copy, i] = act


def act_of(parts):
    blocks, count, width = parts.shape
    return pl.pallas_call(
        act_kernel,
        out_shape=jax.ShapeDtypeStruct((blocks, SPAN, count, width // (2 * SPAN)), BF),
        in_specs=[pl.BlockSpec(memory_space=VM)],
        out_specs=pl.BlockSpec(memory_space=VM),
        compiler_params=pltpu.CompilerParams(vmem_limit_bytes=24 << 20),
        name="act",
    )(parts)


def down_kernel(at_ref, act_ref, own_ref, other_ref, out_ref):
    blocks, width, part = own_ref.shape
    val = None
    for slot, weights_ref in enumerate((own_ref, other_ref)):
        rows = jnp.concatenate([act_ref[at_ref[i], slot] for i in range(blocks)], axis=1)
        more = jnp.dot(rows, weights_ref[...].reshape(blocks * width, part), preferred_element_type=F32)
        val = more if val is None else val + more
    out_ref[...] = val.astype(BF)


def down_of(at, act, own, other):
    return pl.pallas_call(
        down_kernel,
        out_shape=jax.ShapeDtypeStruct((act.shape[2], own.shape[2]), BF),
        in_specs=[pl.BlockSpec(memory_space=pltpu.MemorySpace.SMEM)] + [pl.BlockSpec(memory_space=VM)] * 3,
        out_specs=pl.BlockSpec(memory_space=VM),
        compiler_params=pltpu.CompilerParams(vmem_limit_bytes=24 << 20),
        name="down",
    )(at, act, own, other)


def combine_kernel(back_ref, weight_ref, out_ref):
    experts = back_ref.shape[0]
    weight = weight_ref[...]
    high = weight.astype(BF)
    rest = weight - high.astype(F32)
    middle = rest.astype(BF)
    low = (rest - middle.astype(F32)).astype(BF)
    over_rows = (((0,), (0,)), ((), ()))
    rows = jnp.concatenate([back_ref[e].astype(F32) for e in range(experts)], axis=0).astype(BF)
    val = None
    for term in (low, middle, high):
        more = lax.dot_general(term, rows, over_rows, preferred_element_type=F32)
        val = more if val is None else val + more
    out_ref[...] = val.astype(BF)


def combine(back, weight):
    return pl.pallas_call(
        combine_kernel,
        out_shape=jax.ShapeDtypeStruct((weight.shape[1], back.shape[2]), BF),
        in_specs=[pl.BlockSpec(memory_space=VM)] * 2,
        out_specs=pl.BlockSpec(memory_space=VM),
        compiler_params=pltpu.CompilerParams(vmem_limit_bytes=24 << 20),
        name="combine",
    )(back, weight)


def body(tokens, expert_ids, router_scores, gate_weight, up_weight, down_weight):
    slots, columns = lax.axis_size("expert"), lax.axis_size("hidden")
    experts = slots // SPAN
    part = tokens.shape[1] // columns
    x = lax.axis_index("hidden").astype(jnp.int32)
    same_core = [[SPAN * z + core for z in range(experts)] for core in range(SPAN)]
    swap = [(i, i ^ 1) for i in range(slots)]

    def turned(v, s):
        return lax.ppermute(v, "hidden", [(i, (i + s) % columns) for i in range(columns)])

    def swapped(v):
        return lax.ppermute(v, "expert", swap)

    def exchanged(v):
        return lax.all_to_all(
            v, "expert", split_axis=0, concat_axis=0, tiled=True, axis_index_groups=same_core
        )

    def over_columns(v):
        return lax.all_to_all(v, "hidden", split_axis=0, concat_axis=0, tiled=True)

    downs, others = [], []
    for s in range(columns):
        at = (x + s) % columns * part
        share = lax.dynamic_slice_in_dim(down_weight[0], at, part, 1)
        both = jnp.stack([lax.dynamic_slice_in_dim(w[0], at, part, 0) for w in (gate_weight, up_weight)])
        downs.append(turned(share, s) if s else share)
        others.append(turned(both, s) if s else both)
    down = jnp.stack(downs)
    wide = jnp.stack(others)
    wide_other = swapped(wide)
    down_other = swapped(down)
    outgoing, weight = pack(x.reshape(1), expert_ids.T, router_scores.T, tokens, experts, part)
    own = exchanged(outgoing).reshape(experts * CAP, part)
    source = (x - jnp.arange(columns, dtype=jnp.int32)) % columns
    parts = over_columns(partial_of(source, own, wide, wide_other))
    act_all = over_columns(act_of(parts))
    val = down_of(source, act_all, down, down_other)
    back = exchanged(val.reshape(experts, CAP, part))
    return combine(back, weight)


def solution(mesh):
    return jax.shard_map(
        body,
        mesh=mesh,
        in_specs=(
            P(("groups", "expert"), None),
            P(("groups", "expert"), None),
            P(("groups", "expert"), None),
            P("expert", None, "hidden"),
            P("expert", None, "hidden"),
            P("expert", "hidden", None),
        ),
        out_specs=P(("groups", "expert"), "hidden"),
        check_vma=False,
    )
```

```python
import jax
import jax.numpy as jnp
from jax import lax
from jax.experimental import pallas as pl
from jax.experimental.pallas import tpu as pltpu
from jax.sharding import PartitionSpec as P


SPAN = 2
CAP = 8
F32 = jnp.float32
BF = jnp.bfloat16
VM = pltpu.MemorySpace.VMEM


def stride(experts):
    return max(1, experts // 2 - 1)


def pack_kernel(x_ref, ids_ref, scores_ref, tok_ref, out_ref, weight_ref):
    top, count = ids_ref.shape
    experts, cap, part = out_ref.shape
    pairs = experts * cap
    scores = scores_ref[...]
    routed = 2.5 * scores / jnp.sum(scores, axis=0, keepdims=True)
    row = lax.broadcasted_iota(jnp.int32, (pairs, count), 0)
    expert = row // cap * stride(experts) % experts
    member = jnp.zeros((pairs, count), F32)
    weight = jnp.zeros((pairs, count), F32)
    for k in range(top):
        hit = ids_ref[k : k + 1, :] == expert
        member = jnp.where(hit, 1.0, member)
        weight = jnp.where(hit, routed[k : k + 1, :], weight)
    earlier = lax.broadcasted_iota(jnp.int32, (count, count), 0) < lax.broadcasted_iota(
        jnp.int32, (count, count), 1
    )
    place = jnp.dot(
        member.astype(BF), jnp.where(earlier, 1.0, 0.0).astype(BF), preferred_element_type=F32
    )
    mine = (member > 0.5) & (place == (row % cap).astype(F32))
    weight_ref[...] = jnp.where(mine, weight, 0.0)
    chosen = jnp.where(mine, 1.0, 0.0).astype(BF)
    col = pl.multiple_of(x_ref[0] * part, part)
    rows = jnp.dot(chosen, tok_ref[:, pl.ds(col, part)], preferred_element_type=F32)
    for e in range(experts):
        out_ref[e] = rows[e * cap : (e + 1) * cap].astype(BF)


def pack(x, ids, scores, tokens, experts, part):
    count = tokens.shape[0]
    return pl.pallas_call(
        pack_kernel,
        out_shape=(
            jax.ShapeDtypeStruct((experts, CAP, part), BF),
            jax.ShapeDtypeStruct((experts * CAP, count), F32),
        ),
        in_specs=[pl.BlockSpec(memory_space=pltpu.MemorySpace.SMEM)] + [pl.BlockSpec(memory_space=VM)] * 3,
        out_specs=[pl.BlockSpec(memory_space=VM)] * 2,
        compiler_params=pltpu.CompilerParams(vmem_limit_bytes=24 << 20),
        name="pack",
    )(x, ids, scores, tokens)


def partial_kernel(at_ref, rows_ref, own_ref, other_ref, out_ref):
    rows = rows_ref[...]
    for s in range(own_ref.shape[0]):
        weights = jnp.concatenate([r[s, i] for r in (own_ref, other_ref) for i in range(2)], axis=1)
        out_ref[at_ref[s]] = jnp.dot(rows, weights, preferred_element_type=F32).astype(BF)


def partial_of(at, rows, own, other):
    blocks, _, _, width = own.shape
    return pl.pallas_call(
        partial_kernel,
        out_shape=jax.ShapeDtypeStruct((blocks, rows.shape[0], 2 * SPAN * width), BF),
        in_specs=[pl.BlockSpec(memory_space=pltpu.MemorySpace.SMEM)] + [pl.BlockSpec(memory_space=VM)] * 3,
        out_specs=pl.BlockSpec(memory_space=VM),
        compiler_params=pltpu.CompilerParams(vmem_limit_bytes=24 << 20),
        name="partial",
    )(at, rows, own, other)


def act_kernel(parts_ref, out_ref):
    blocks = parts_ref.shape[0]
    width = out_ref.shape[3]
    val = parts_ref[0].astype(F32)
    for i in range(1, blocks):
        val = val + parts_ref[i].astype(F32)
    for i in range(SPAN):
        gate = val[:, 2 * i * width : (2 * i + 1) * width]
        up = val[:, (2 * i + 1) * width : (2 * i + 2) * width]
        act = (gate / (1.0 + jnp.exp(-gate)) * up).astype(BF)
        for copy in range(blocks):
            out_ref[copy, i] = act


def act_of(parts):
    blocks, count, width = parts.shape
    return pl.pallas_call(
        act_kernel,
        out_shape=jax.ShapeDtypeStruct((blocks, SPAN, count, width // (2 * SPAN)), BF),
        in_specs=[pl.BlockSpec(memory_space=VM)],
        out_specs=pl.BlockSpec(memory_space=VM),
        compiler_params=pltpu.CompilerParams(vmem_limit_bytes=24 << 20),
        name="act",
    )(parts)


def down_kernel(at_ref, act_ref, own_ref, other_ref, out_ref):
    blocks, width, part = own_ref.shape
    val = None
    for slot, weights_ref in enumerate((own_ref, other_ref)):
        rows = jnp.concatenate([act_ref[at_ref[i], slot] for i in range(blocks)], axis=1)
        more = jnp.dot(rows, weights_ref[...].reshape(blocks * width, part), preferred_element_type=F32)
        val = more if val is None else val + more
    out_ref[...] = val.astype(BF)


def down_of(at, act, own, other):
    return pl.pallas_call(
        down_kernel,
        out_shape=jax.ShapeDtypeStruct((act.shape[2], own.shape[2]), BF),
        in_specs=[pl.BlockSpec(memory_space=pltpu.MemorySpace.SMEM)] + [pl.BlockSpec(memory_space=VM)] * 3,
        out_specs=pl.BlockSpec(memory_space=VM),
        compiler_params=pltpu.CompilerParams(vmem_limit_bytes=24 << 20),
        name="down",
    )(at, act, own, other)


def combine_kernel(back_ref, weight_ref, out_ref):
    experts = back_ref.shape[0]
    weight = weight_ref[...]
    high = weight.astype(BF)
    rest = weight - high.astype(F32)
    middle = rest.astype(BF)
    low = (rest - middle.astype(F32)).astype(BF)
    over_rows = (((0,), (0,)), ((), ()))
    rows = jnp.concatenate([back_ref[e].astype(F32) for e in range(experts)], axis=0).astype(BF)
    val = None
    for term in (low, middle, high):
        more = lax.dot_general(term, rows, over_rows, preferred_element_type=F32)
        val = more if val is None else val + more
    out_ref[...] = val.astype(BF)


def combine(back, weight):
    return pl.pallas_call(
        combine_kernel,
        out_shape=jax.ShapeDtypeStruct((weight.shape[1], back.shape[2]), BF),
        in_specs=[pl.BlockSpec(memory_space=VM)] * 2,
        out_specs=pl.BlockSpec(memory_space=VM),
        compiler_params=pltpu.CompilerParams(vmem_limit_bytes=24 << 20),
        name="combine",
    )(back, weight)


def body(tokens, expert_ids, router_scores, gate_weight, up_weight, down_weight):
    slots, columns = lax.axis_size("expert"), lax.axis_size("hidden")
    experts = slots // SPAN
    part = tokens.shape[1] // columns
    x = lax.axis_index("hidden").astype(jnp.int32)
    order = [j * stride(experts) % experts for j in range(experts)]
    same_core = [[SPAN * z + core for z in order] for core in range(SPAN)]
    swap = [(i, i ^ 1) for i in range(slots)]

    def turned(v, s):
        return lax.ppermute(v, "hidden", [(i, (i + s) % columns) for i in range(columns)])

    def swapped(v):
        return lax.ppermute(v, "expert", swap)

    def exchanged(v):
        return lax.all_to_all(
            v, "expert", split_axis=0, concat_axis=0, tiled=True, axis_index_groups=same_core
        )

    def over_columns(v):
        return lax.all_to_all(v, "hidden", split_axis=0, concat_axis=0, tiled=True)

    downs, others = [], []
    for s in range(columns):
        at = (x + s) % columns * part
        share = lax.dynamic_slice_in_dim(down_weight[0], at, part, 1)
        both = jnp.stack([lax.dynamic_slice_in_dim(w[0], at, part, 0) for w in (gate_weight, up_weight)])
        downs.append(turned(share, s) if s else share)
        others.append(turned(both, s) if s else both)
    down = jnp.stack(downs)
    wide = jnp.stack(others)
    wide_other = swapped(wide)
    down_other = swapped(down)
    outgoing, weight = pack(x.reshape(1), expert_ids.T, router_scores.T, tokens, experts, part)
    own = exchanged(outgoing).reshape(experts * CAP, part)
    source = (x - jnp.arange(columns, dtype=jnp.int32)) % columns
    parts = over_columns(partial_of(source, own, wide, wide_other))
    act_all = over_columns(act_of(parts))
    val = down_of(source, act_all, down, down_other)
    back = exchanged(val.reshape(experts, CAP, part))
    return combine(back, weight)


def solution(mesh):
    return jax.shard_map(
        body,
        mesh=mesh,
        in_specs=(
            P(("groups", "expert"), None),
            P(("groups", "expert"), None),
            P(("groups", "expert"), None),
            P("expert", None, "hidden"),
            P("expert", None, "hidden"),
            P("expert", "hidden", None),
        ),
        out_specs=P(("groups", "expert"), "hidden"),
        check_vma=False,
    )
```

```python
import jax
import jax.numpy as jnp
from jax import lax
from jax.experimental import pallas as pl
from jax.experimental.pallas import tpu as pltpu
from jax.sharding import PartitionSpec as P


SPAN = 2
CAP = 8
F32 = jnp.float32
BF = jnp.bfloat16
VM = pltpu.MemorySpace.VMEM
HB = pltpu.MemorySpace.HBM


def stride(experts):
    return max(1, experts // 2 - 1)


def pack_kernel(x_ref, ids_hbm, scores_hbm, tok_hbm, out_ref, weight_ref, ids_ref, scores_ref, tok_ref, sems):
    width = tok_ref.shape[1]
    col = pl.multiple_of(x_ref[0] * width, width)
    copies = [
        pltpu.make_async_copy(ids_hbm, ids_ref, sems.at[0]),
        pltpu.make_async_copy(scores_hbm, scores_ref, sems.at[1]),
        pltpu.make_async_copy(tok_hbm.at[:, pl.ds(col, width)], tok_ref, sems.at[2]),
    ]
    for copy in copies:
        copy.start()
    for copy in copies:
        copy.wait()
    top, count = ids_ref.shape
    experts, cap, _ = out_ref.shape
    pairs = experts * cap
    scores = scores_ref[...]
    routed = 2.5 * scores / jnp.sum(scores, axis=0, keepdims=True)
    row = lax.broadcasted_iota(jnp.int32, (pairs, count), 0)
    expert = row // cap * stride(experts) % experts
    member = jnp.zeros((pairs, count), F32)
    weight = jnp.zeros((pairs, count), F32)
    for k in range(top):
        hit = ids_ref[k : k + 1, :] == expert
        member = jnp.where(hit, 1.0, member)
        weight = jnp.where(hit, routed[k : k + 1, :], weight)
    earlier = lax.broadcasted_iota(jnp.int32, (count, count), 0) < lax.broadcasted_iota(
        jnp.int32, (count, count), 1
    )
    place = jnp.dot(
        member.astype(BF), jnp.where(earlier, 1.0, 0.0).astype(BF), preferred_element_type=F32
    )
    mine = (member > 0.5) & (place == (row % cap).astype(F32))
    weight_ref[...] = jnp.where(mine, weight, 0.0)
    chosen = jnp.where(mine, 1.0, 0.0).astype(BF)
    rows = jnp.dot(chosen, tok_ref[...], preferred_element_type=F32)
    for e in range(experts):
        out_ref[e] = rows[e * cap : (e + 1) * cap].astype(BF)


def pack(x, ids, scores, tokens, experts, part):
    count = tokens.shape[0]
    return pl.pallas_call(
        pack_kernel,
        out_shape=(
            jax.ShapeDtypeStruct((experts, CAP, part), BF),
            jax.ShapeDtypeStruct((experts * CAP, count), F32),
        ),
        in_specs=[pl.BlockSpec(memory_space=pltpu.MemorySpace.SMEM)] + [pl.BlockSpec(memory_space=HB)] * 3,
        out_specs=[pl.BlockSpec(memory_space=VM)] * 2,
        scratch_shapes=[
            pltpu.VMEM(ids.shape, ids.dtype),
            pltpu.VMEM(scores.shape, scores.dtype),
            pltpu.VMEM((count, part), tokens.dtype),
            pltpu.SemaphoreType.DMA((3,)),
        ],
        name="pack",
    )(x, ids, scores, tokens)


def partial_kernel(at_ref, rows_ref, own_ref, other_hbm, out_hbm, other_ref, out_ref, sem, sems):
    fetch = pltpu.make_async_copy(other_hbm, other_ref, sem)
    fetch.start()
    rows = rows_ref[...]
    blocks, _, _, width = own_ref.shape

    def product(weights_ref, s):
        weights = jnp.concatenate([weights_ref[s, i] for i in range(2)], axis=1)
        return jnp.dot(rows, weights, preferred_element_type=F32).astype(BF)

    for s in range(blocks):
        out_ref[s, :, : 2 * width] = product(own_ref, s)
    fetch.wait()
    stores = []
    for s in range(blocks):
        out_ref[s, :, 2 * width :] = product(other_ref, s)
        stores.append(pltpu.make_async_copy(out_ref.at[s], out_hbm.at[at_ref[s]], sems.at[s]))
        stores[-1].start()
    for store in stores:
        store.wait()


def partial_of(at, rows, own, other):
    blocks, _, _, width = own.shape
    shape = (blocks, rows.shape[0], 2 * SPAN * width)
    return pl.pallas_call(
        partial_kernel,
        out_shape=pltpu.MemorySpace.HBM(shape, BF),
        in_specs=[
            pl.BlockSpec(memory_space=pltpu.MemorySpace.SMEM),
            pl.BlockSpec(memory_space=VM),
            pl.BlockSpec(memory_space=VM),
            pl.BlockSpec(memory_space=HB),
        ],
        out_specs=pl.BlockSpec(memory_space=HB),
        scratch_shapes=[
            pltpu.VMEM(other.shape, BF),
            pltpu.VMEM(shape, BF),
            pltpu.SemaphoreType.DMA,
            pltpu.SemaphoreType.DMA((blocks,)),
        ],
        compiler_params=pltpu.CompilerParams(vmem_limit_bytes=24 << 20),
        name="partial",
    )(at, rows, own, pltpu.with_memory_space_constraint(other, pltpu.MemorySpace.HBM))


def act_kernel(parts_ref, out_ref):
    blocks = parts_ref.shape[0]
    width = out_ref.shape[3]
    val = parts_ref[0].astype(F32)
    for i in range(1, blocks):
        val = val + parts_ref[i].astype(F32)
    for i in range(SPAN):
        gate = val[:, 2 * i * width : (2 * i + 1) * width]
        up = val[:, (2 * i + 1) * width : (2 * i + 2) * width]
        act = (gate / (1.0 + jnp.exp(-gate)) * up).astype(BF)
        for copy in range(blocks):
            out_ref[copy, i] = act


def act_of(parts):
    blocks, count, width = parts.shape
    return pl.pallas_call(
        act_kernel,
        out_shape=jax.ShapeDtypeStruct((blocks, SPAN, count, width // (2 * SPAN)), BF),
        in_specs=[pl.BlockSpec(memory_space=VM)],
        out_specs=pl.BlockSpec(memory_space=VM),
        compiler_params=pltpu.CompilerParams(vmem_limit_bytes=24 << 20),
        name="act",
    )(parts)


def down_kernel(at_ref, act_ref, own_ref, other_ref, out_ref):
    blocks, width, part = own_ref.shape
    val = None
    for slot, weights_ref in enumerate((own_ref, other_ref)):
        rows = jnp.concatenate([act_ref[at_ref[i], slot] for i in range(blocks)], axis=1)
        more = jnp.dot(rows, weights_ref[...].reshape(blocks * width, part), preferred_element_type=F32)
        val = more if val is None else val + more
    out_ref[...] = val.astype(BF)


def down_of(at, act, own, other):
    return pl.pallas_call(
        down_kernel,
        out_shape=jax.ShapeDtypeStruct((act.shape[2], own.shape[2]), BF),
        in_specs=[pl.BlockSpec(memory_space=pltpu.MemorySpace.SMEM)] + [pl.BlockSpec(memory_space=VM)] * 3,
        out_specs=pl.BlockSpec(memory_space=VM),
        compiler_params=pltpu.CompilerParams(vmem_limit_bytes=24 << 20),
        name="down",
    )(at, act, own, other)


def combine_kernel(back_ref, weight_ref, out_ref):
    experts = back_ref.shape[0]
    weight = weight_ref[...]
    high = weight.astype(BF)
    rest = weight - high.astype(F32)
    middle = rest.astype(BF)
    low = (rest - middle.astype(F32)).astype(BF)
    over_rows = (((0,), (0,)), ((), ()))
    rows = jnp.concatenate([back_ref[e].astype(F32) for e in range(experts)], axis=0).astype(BF)
    val = None
    for term in (low, middle, high):
        more = lax.dot_general(term, rows, over_rows, preferred_element_type=F32)
        val = more if val is None else val + more
    out_ref[...] = val.astype(BF)


def combine(back, weight):
    return pl.pallas_call(
        combine_kernel,
        out_shape=jax.ShapeDtypeStruct((weight.shape[1], back.shape[2]), BF),
        in_specs=[pl.BlockSpec(memory_space=VM)] * 2,
        out_specs=pl.BlockSpec(memory_space=VM),
        compiler_params=pltpu.CompilerParams(vmem_limit_bytes=24 << 20),
        name="combine",
    )(back, weight)


def body(tokens, expert_ids, router_scores, gate_weight, up_weight, down_weight):
    slots, columns = lax.axis_size("expert"), lax.axis_size("hidden")
    experts = slots // SPAN
    part = tokens.shape[1] // columns
    x = lax.axis_index("hidden").astype(jnp.int32)
    order = [j * stride(experts) % experts for j in range(experts)]
    same_core = [[SPAN * z + core for z in order] for core in range(SPAN)]
    swap = [(i, i ^ 1) for i in range(slots)]

    def turned(v, s):
        return lax.ppermute(v, "hidden", [(i, (i + s) % columns) for i in range(columns)])

    def swapped(v):
        return lax.ppermute(v, "expert", swap)

    def exchanged(v):
        return lax.all_to_all(
            v, "expert", split_axis=0, concat_axis=0, tiled=True, axis_index_groups=same_core
        )

    def over_columns(v):
        return lax.all_to_all(v, "hidden", split_axis=0, concat_axis=0, tiled=True)

    downs, others = [], []
    for s in range(columns):
        at = (x + s) % columns * part
        share = lax.dynamic_slice_in_dim(down_weight[0], at, part, 1)
        both = jnp.stack([lax.dynamic_slice_in_dim(w[0], at, part, 0) for w in (gate_weight, up_weight)])
        downs.append(turned(share, s) if s else share)
        others.append(turned(both, s) if s else both)
    down = jnp.stack(downs)
    wide = jnp.stack(others)
    wide_other = swapped(wide)
    down_other = swapped(down)
    outgoing, weight = pack(x.reshape(1), expert_ids.T, router_scores.T, tokens, experts, part)
    own = exchanged(outgoing).reshape(experts * CAP, part)
    source = (x - jnp.arange(columns, dtype=jnp.int32)) % columns
    parts = over_columns(partial_of(source, own, wide, wide_other))
    act_all = over_columns(act_of(parts))
    val = down_of(source, act_all, down, down_other)
    back = exchanged(val.reshape(experts, CAP, part))
    return combine(back, weight)


def solution(mesh):
    return jax.shard_map(
        body,
        mesh=mesh,
        in_specs=(
            P(("groups", "expert"), None),
            P(("groups", "expert"), None),
            P(("groups", "expert"), None),
            P("expert", None, "hidden"),
            P("expert", None, "hidden"),
            P("expert", "hidden", None),
        ),
        out_specs=P(("groups", "expert"), "hidden"),
        check_vma=False,
    )
```

```python
import jax
import jax.numpy as jnp
from jax import lax
from jax.experimental import pallas as pl
from jax.experimental.pallas import tpu as pltpu
from jax.sharding import PartitionSpec as P


SPAN = 2
CAP = 8
F32 = jnp.float32
BF = jnp.bfloat16
VM = pltpu.MemorySpace.VMEM
HB = pltpu.MemorySpace.HBM


def stride(experts):
    return max(1, experts // 2 - 1)


def pack_kernel(x_ref, ids_hbm, scores_hbm, tok_hbm, out_ref, weight_ref, ids_ref, scores_ref, tok_ref, sems):
    width = tok_ref.shape[1]
    col = pl.multiple_of(x_ref[0] * width, width)
    copies = [
        pltpu.make_async_copy(ids_hbm, ids_ref, sems.at[0]),
        pltpu.make_async_copy(scores_hbm, scores_ref, sems.at[1]),
        pltpu.make_async_copy(tok_hbm.at[:, pl.ds(col, width)], tok_ref, sems.at[2]),
    ]
    for copy in copies:
        copy.start()
    for copy in copies:
        copy.wait()
    top, count = ids_ref.shape
    experts, cap, _ = out_ref.shape
    pairs = experts * cap
    scores = scores_ref[...]
    routed = 2.5 * scores / jnp.sum(scores, axis=0, keepdims=True)
    row = lax.broadcasted_iota(jnp.int32, (pairs, count), 0)
    expert = row // cap * x_ref[1] % experts
    member = jnp.zeros((pairs, count), F32)
    weight = jnp.zeros((pairs, count), F32)
    for k in range(top):
        hit = ids_ref[k : k + 1, :] == expert
        member = jnp.where(hit, 1.0, member)
        weight = jnp.where(hit, routed[k : k + 1, :], weight)
    earlier = lax.broadcasted_iota(jnp.int32, (count, count), 0) < lax.broadcasted_iota(
        jnp.int32, (count, count), 1
    )
    place = jnp.dot(
        member.astype(BF), jnp.where(earlier, 1.0, 0.0).astype(BF), preferred_element_type=F32
    )
    mine = (member > 0.5) & (place == (row % cap).astype(F32))
    weight_ref[...] = jnp.where(mine, weight, 0.0)
    chosen = jnp.where(mine, 1.0, 0.0).astype(BF)
    rows = jnp.dot(chosen, tok_ref[...], preferred_element_type=F32)
    for e in range(experts):
        out_ref[e] = rows[e * cap : (e + 1) * cap].astype(BF)


def pack(x, ids, scores, tokens, experts, part):
    count = tokens.shape[0]
    return pl.pallas_call(
        pack_kernel,
        out_shape=(
            jax.ShapeDtypeStruct((experts, CAP, part), BF),
            jax.ShapeDtypeStruct((experts * CAP, count), F32),
        ),
        in_specs=[pl.BlockSpec(memory_space=pltpu.MemorySpace.SMEM)] + [pl.BlockSpec(memory_space=HB)] * 3,
        out_specs=[pl.BlockSpec(memory_space=VM)] * 2,
        scratch_shapes=[
            pltpu.VMEM(ids.shape, ids.dtype),
            pltpu.VMEM(scores.shape, scores.dtype),
            pltpu.VMEM((count, part), tokens.dtype),
            pltpu.SemaphoreType.DMA((3,)),
        ],
        name="pack",
    )(x, ids, scores, tokens)


def partial_kernel(at_ref, rows_ref, own_ref, other_hbm, out_hbm, other_ref, out_ref, sem, sems):
    fetch = pltpu.make_async_copy(other_hbm, other_ref, sem)
    fetch.start()
    rows = rows_ref[...]
    blocks, _, _, width = own_ref.shape

    def product(weights_ref, s):
        weights = jnp.concatenate([weights_ref[s, i] for i in range(2)], axis=1)
        return jnp.dot(rows, weights, preferred_element_type=F32).astype(BF)

    for s in range(blocks):
        out_ref[s, :, : 2 * width] = product(own_ref, s)
    fetch.wait()
    stores = []
    for s in range(blocks):
        out_ref[s, :, 2 * width :] = product(other_ref, s)
        stores.append(pltpu.make_async_copy(out_ref.at[s], out_hbm.at[at_ref[s]], sems.at[s]))
        stores[-1].start()
    for store in stores:
        store.wait()


def partial_of(at, rows, own, other):
    blocks, _, _, width = own.shape
    shape = (blocks, rows.shape[0], 2 * SPAN * width)
    return pl.pallas_call(
        partial_kernel,
        out_shape=pltpu.MemorySpace.HBM(shape, BF),
        in_specs=[
            pl.BlockSpec(memory_space=pltpu.MemorySpace.SMEM),
            pl.BlockSpec(memory_space=VM),
            pl.BlockSpec(memory_space=VM),
            pl.BlockSpec(memory_space=HB),
        ],
        out_specs=pl.BlockSpec(memory_space=HB),
        scratch_shapes=[
            pltpu.VMEM(other.shape, BF),
            pltpu.VMEM(shape, BF),
            pltpu.SemaphoreType.DMA,
            pltpu.SemaphoreType.DMA((blocks,)),
        ],
        compiler_params=pltpu.CompilerParams(vmem_limit_bytes=24 << 20),
        name="partial",
    )(at, rows, own, pltpu.with_memory_space_constraint(other, pltpu.MemorySpace.HBM))


def act_kernel(parts_ref, out_ref):
    blocks = parts_ref.shape[0]
    width = out_ref.shape[3]
    val = parts_ref[0].astype(F32)
    for i in range(1, blocks):
        val = val + parts_ref[i].astype(F32)
    for i in range(SPAN):
        gate = val[:, 2 * i * width : (2 * i + 1) * width]
        up = val[:, (2 * i + 1) * width : (2 * i + 2) * width]
        act = (gate / (1.0 + jnp.exp(-gate)) * up).astype(BF)
        for copy in range(blocks):
            out_ref[copy, i] = act


def act_of(parts):
    blocks, count, width = parts.shape
    return pl.pallas_call(
        act_kernel,
        out_shape=jax.ShapeDtypeStruct((blocks, SPAN, count, width // (2 * SPAN)), BF),
        in_specs=[pl.BlockSpec(memory_space=VM)],
        out_specs=pl.BlockSpec(memory_space=VM),
        compiler_params=pltpu.CompilerParams(vmem_limit_bytes=24 << 20),
        name="act",
    )(parts)


def down_kernel(at_ref, act_ref, own_ref, other_ref, out_ref):
    blocks, width, part = own_ref.shape
    val = None
    for slot, weights_ref in enumerate((own_ref, other_ref)):
        rows = jnp.concatenate([act_ref[at_ref[i], slot] for i in range(blocks)], axis=1)
        more = jnp.dot(rows, weights_ref[...].reshape(blocks * width, part), preferred_element_type=F32)
        val = more if val is None else val + more
    out_ref[...] = val.astype(BF)


def down_of(at, act, own, other):
    return pl.pallas_call(
        down_kernel,
        out_shape=jax.ShapeDtypeStruct((act.shape[2], own.shape[2]), BF),
        in_specs=[pl.BlockSpec(memory_space=pltpu.MemorySpace.SMEM)] + [pl.BlockSpec(memory_space=VM)] * 3,
        out_specs=pl.BlockSpec(memory_space=VM),
        compiler_params=pltpu.CompilerParams(vmem_limit_bytes=24 << 20),
        name="down",
    )(at, act, own, other)


def combine_kernel(back_ref, weight_ref, out_ref):
    experts = back_ref.shape[0]
    weight = weight_ref[...]
    high = weight.astype(BF)
    rest = weight - high.astype(F32)
    middle = rest.astype(BF)
    low = (rest - middle.astype(F32)).astype(BF)
    over_rows = (((0,), (0,)), ((), ()))
    rows = jnp.concatenate([back_ref[e].astype(F32) for e in range(experts)], axis=0).astype(BF)
    val = None
    for term in (low, middle, high):
        more = lax.dot_general(term, rows, over_rows, preferred_element_type=F32)
        val = more if val is None else val + more
    out_ref[...] = val.astype(BF)


def combine(back, weight):
    return pl.pallas_call(
        combine_kernel,
        out_shape=jax.ShapeDtypeStruct((weight.shape[1], back.shape[2]), BF),
        in_specs=[pl.BlockSpec(memory_space=VM)] * 2,
        out_specs=pl.BlockSpec(memory_space=VM),
        compiler_params=pltpu.CompilerParams(vmem_limit_bytes=24 << 20),
        name="combine",
    )(back, weight)


def body(tokens, expert_ids, router_scores, gate_weight, up_weight, down_weight):
    slots, columns = lax.axis_size("expert"), lax.axis_size("hidden")
    experts = slots // SPAN
    part = tokens.shape[1] // columns
    x = lax.axis_index("hidden").astype(jnp.int32)
    steps = [stride(experts), experts - stride(experts)]
    same_core = [[SPAN * (j * steps[c] % experts) + c for j in range(experts)] for c in range(SPAN)]
    core = (lax.axis_index("expert") % SPAN).astype(jnp.int32)
    step = jnp.where(core == 0, steps[0], steps[1]).astype(jnp.int32)
    swap = [(i, i ^ 1) for i in range(slots)]

    def turned(v, s):
        return lax.ppermute(v, "hidden", [(i, (i + s) % columns) for i in range(columns)])

    def swapped(v):
        return lax.ppermute(v, "expert", swap)

    def exchanged(v):
        return lax.all_to_all(
            v, "expert", split_axis=0, concat_axis=0, tiled=True, axis_index_groups=same_core
        )

    def over_columns(v):
        return lax.all_to_all(v, "hidden", split_axis=0, concat_axis=0, tiled=True)

    downs, others = [], []
    for s in range(columns):
        at = (x + s) % columns * part
        share = lax.dynamic_slice_in_dim(down_weight[0], at, part, 1)
        both = jnp.stack([lax.dynamic_slice_in_dim(w[0], at, part, 0) for w in (gate_weight, up_weight)])
        downs.append(turned(share, s) if s else share)
        others.append(turned(both, s) if s else both)
    down = jnp.stack(downs)
    wide = jnp.stack(others)
    wide_other = swapped(wide)
    down_other = swapped(down)
    outgoing, weight = pack(jnp.stack([x, step]), expert_ids.T, router_scores.T, tokens, experts, part)
    own = exchanged(outgoing).reshape(experts * CAP, part)
    source = (x - jnp.arange(columns, dtype=jnp.int32)) % columns
    parts = over_columns(partial_of(source, own, wide, wide_other))
    act_all = over_columns(act_of(parts))
    val = down_of(source, act_all, down, down_other)
    back = exchanged(val.reshape(experts, CAP, part))
    return combine(back, weight)


def solution(mesh):
    return jax.shard_map(
        body,
        mesh=mesh,
        in_specs=(
            P(("groups", "expert"), None),
            P(("groups", "expert"), None),
            P(("groups", "expert"), None),
            P("expert", None, "hidden"),
            P("expert", None, "hidden"),
            P("expert", "hidden", None),
        ),
        out_specs=P(("groups", "expert"), "hidden"),
        check_vma=False,
    )
```

```python
import jax
import jax.numpy as jnp
from jax import lax
from jax.experimental import pallas as pl
from jax.experimental.pallas import tpu as pltpu
from jax.sharding import PartitionSpec as P


SPAN = 2
CAP = 8
F32 = jnp.float32
BF = jnp.bfloat16
VM = pltpu.MemorySpace.VMEM
HB = pltpu.MemorySpace.HBM


def stride(experts):
    return max(1, experts // 2 - 1)


def pack_kernel(x_ref, ids_hbm, scores_hbm, tok_hbm, out_ref, weight_ref, ids_ref, scores_ref, tok_ref, sems):
    width = tok_ref.shape[1]
    col = pl.multiple_of(x_ref[0] * width, width)
    copies = [
        pltpu.make_async_copy(ids_hbm, ids_ref, sems.at[0]),
        pltpu.make_async_copy(scores_hbm, scores_ref, sems.at[1]),
        pltpu.make_async_copy(tok_hbm.at[:, pl.ds(col, width)], tok_ref, sems.at[2]),
    ]
    for copy in copies:
        copy.start()
    for copy in copies:
        copy.wait()
    top, count = ids_ref.shape
    experts, cap, _ = out_ref.shape
    pairs = experts * cap
    scores = scores_ref[...]
    routed = 2.5 * scores / jnp.sum(scores, axis=0, keepdims=True)
    row = lax.broadcasted_iota(jnp.int32, (pairs, count), 0)
    expert = row // cap * stride(experts) % experts
    member = jnp.zeros((pairs, count), F32)
    weight = jnp.zeros((pairs, count), F32)
    for k in range(top):
        hit = ids_ref[k : k + 1, :] == expert
        member = jnp.where(hit, 1.0, member)
        weight = jnp.where(hit, routed[k : k + 1, :], weight)
    earlier = lax.broadcasted_iota(jnp.int32, (count, count), 0) < lax.broadcasted_iota(
        jnp.int32, (count, count), 1
    )
    place = jnp.dot(
        member.astype(BF), jnp.where(earlier, 1.0, 0.0).astype(BF), preferred_element_type=F32
    )
    mine = (member > 0.5) & (place == (row % cap).astype(F32))
    weight_ref[...] = jnp.where(mine, weight, 0.0)
    chosen = jnp.where(mine, 1.0, 0.0).astype(BF)
    rows = jnp.dot(chosen, tok_ref[...], preferred_element_type=F32)
    for e in range(experts):
        out_ref[e] = rows[e * cap : (e + 1) * cap].astype(BF)


def pack(x, ids, scores, tokens, experts, part):
    count = tokens.shape[0]
    return pl.pallas_call(
        pack_kernel,
        out_shape=(
            jax.ShapeDtypeStruct((experts, CAP, part), BF),
            jax.ShapeDtypeStruct((experts * CAP, count), F32),
        ),
        in_specs=[pl.BlockSpec(memory_space=pltpu.MemorySpace.SMEM)] + [pl.BlockSpec(memory_space=HB)] * 3,
        out_specs=[pl.BlockSpec(memory_space=VM)] * 2,
        scratch_shapes=[
            pltpu.VMEM(ids.shape, ids.dtype),
            pltpu.VMEM(scores.shape, scores.dtype),
            pltpu.VMEM((count, part), tokens.dtype),
            pltpu.SemaphoreType.DMA((3,)),
        ],
        name="pack",
    )(x, ids, scores, tokens)


def partial_kernel(at_ref, rows_ref, own_ref, other_hbm, out_hbm, other_ref, out_ref, fetch_sems, sems):
    blocks = own_ref.shape[0]
    fetches = [pltpu.make_async_copy(other_hbm.at[s], other_ref.at[s], fetch_sems.at[s]) for s in range(blocks)]
    for fetch in fetches:
        fetch.start()
    rows = rows_ref[...]
    stores = []
    for s in range(blocks):
        fetches[s].wait()
        weights = jnp.concatenate([r[s, i] for r in (own_ref, other_ref) for i in range(2)], axis=1)
        out_ref[s] = jnp.dot(rows, weights, preferred_element_type=F32).astype(BF)
        stores.append(pltpu.make_async_copy(out_ref.at[s], out_hbm.at[at_ref[s]], sems.at[s]))
        stores[-1].start()
    for store in stores:
        store.wait()


def partial_of(at, rows, own, other):
    blocks, _, _, width = own.shape
    shape = (blocks, rows.shape[0], 2 * SPAN * width)
    return pl.pallas_call(
        partial_kernel,
        out_shape=pltpu.MemorySpace.HBM(shape, BF),
        in_specs=[
            pl.BlockSpec(memory_space=pltpu.MemorySpace.SMEM),
            pl.BlockSpec(memory_space=VM),
            pl.BlockSpec(memory_space=VM),
            pl.BlockSpec(memory_space=HB),
        ],
        out_specs=pl.BlockSpec(memory_space=HB),
        scratch_shapes=[
            pltpu.VMEM(other.shape, BF),
            pltpu.VMEM(shape, BF),
            pltpu.SemaphoreType.DMA((blocks,)),
            pltpu.SemaphoreType.DMA((blocks,)),
        ],
        compiler_params=pltpu.CompilerParams(vmem_limit_bytes=24 << 20),
        name="partial",
    )(at, rows, own, pltpu.with_memory_space_constraint(other, pltpu.MemorySpace.HBM))


def act_kernel(parts_ref, out_ref):
    blocks = parts_ref.shape[0]
    width = out_ref.shape[3]
    val = parts_ref[0].astype(F32)
    for i in range(1, blocks):
        val = val + parts_ref[i].astype(F32)
    for i in range(SPAN):
        gate = val[:, 2 * i * width : (2 * i + 1) * width]
        up = val[:, (2 * i + 1) * width : (2 * i + 2) * width]
        act = (gate / (1.0 + jnp.exp(-gate)) * up).astype(BF)
        for copy in range(blocks):
            out_ref[copy, i] = act


def act_of(parts):
    blocks, count, width = parts.shape
    return pl.pallas_call(
        act_kernel,
        out_shape=jax.ShapeDtypeStruct((blocks, SPAN, count, width // (2 * SPAN)), BF),
        in_specs=[pl.BlockSpec(memory_space=VM)],
        out_specs=pl.BlockSpec(memory_space=VM),
        compiler_params=pltpu.CompilerParams(vmem_limit_bytes=24 << 20),
        name="act",
    )(parts)


def down_kernel(at_ref, act_ref, own_ref, other_ref, out_ref):
    blocks, width, part = own_ref.shape
    val = None
    for slot, weights_ref in enumerate((own_ref, other_ref)):
        rows = jnp.concatenate([act_ref[at_ref[i], slot] for i in range(blocks)], axis=1)
        more = jnp.dot(rows, weights_ref[...].reshape(blocks * width, part), preferred_element_type=F32)
        val = more if val is None else val + more
    out_ref[...] = val.astype(BF)


def down_of(at, act, own, other):
    return pl.pallas_call(
        down_kernel,
        out_shape=jax.ShapeDtypeStruct((act.shape[2], own.shape[2]), BF),
        in_specs=[pl.BlockSpec(memory_space=pltpu.MemorySpace.SMEM)] + [pl.BlockSpec(memory_space=VM)] * 3,
        out_specs=pl.BlockSpec(memory_space=VM),
        compiler_params=pltpu.CompilerParams(vmem_limit_bytes=24 << 20),
        name="down",
    )(at, act, own, other)


def combine_kernel(back_ref, weight_ref, out_ref):
    experts = back_ref.shape[0]
    weight = weight_ref[...]
    high = weight.astype(BF)
    rest = weight - high.astype(F32)
    middle = rest.astype(BF)
    low = (rest - middle.astype(F32)).astype(BF)
    over_rows = (((0,), (0,)), ((), ()))
    rows = jnp.concatenate([back_ref[e].astype(F32) for e in range(experts)], axis=0).astype(BF)
    val = None
    for term in (low, middle, high):
        more = lax.dot_general(term, rows, over_rows, preferred_element_type=F32)
        val = more if val is None else val + more
    out_ref[...] = val.astype(BF)


def combine(back, weight):
    return pl.pallas_call(
        combine_kernel,
        out_shape=jax.ShapeDtypeStruct((weight.shape[1], back.shape[2]), BF),
        in_specs=[pl.BlockSpec(memory_space=VM)] * 2,
        out_specs=pl.BlockSpec(memory_space=VM),
        compiler_params=pltpu.CompilerParams(vmem_limit_bytes=24 << 20),
        name="combine",
    )(back, weight)


def body(tokens, expert_ids, router_scores, gate_weight, up_weight, down_weight):
    slots, columns = lax.axis_size("expert"), lax.axis_size("hidden")
    experts = slots // SPAN
    part = tokens.shape[1] // columns
    x = lax.axis_index("hidden").astype(jnp.int32)
    order = [j * stride(experts) % experts for j in range(experts)]
    same_core = [[SPAN * z + core for z in order] for core in range(SPAN)]
    swap = [(i, i ^ 1) for i in range(slots)]

    def turned(v, s):
        return lax.ppermute(v, "hidden", [(i, (i + s) % columns) for i in range(columns)])

    def swapped(v):
        return lax.ppermute(v, "expert", swap)

    def exchanged(v):
        return lax.all_to_all(
            v, "expert", split_axis=0, concat_axis=0, tiled=True, axis_index_groups=same_core
        )

    def over_columns(v):
        return lax.all_to_all(v, "hidden", split_axis=0, concat_axis=0, tiled=True)

    downs, others = [], []
    for s in range(columns):
        at = (x + s) % columns * part
        share = lax.dynamic_slice_in_dim(down_weight[0], at, part, 1)
        both = jnp.stack([lax.dynamic_slice_in_dim(w[0], at, part, 0) for w in (gate_weight, up_weight)])
        downs.append(turned(share, s) if s else share)
        others.append(turned(both, s) if s else both)
    down = jnp.stack(downs)
    wide = jnp.stack(others)
    wide_other = swapped(wide)
    down_other = swapped(down)
    outgoing, weight = pack(x.reshape(1), expert_ids.T, router_scores.T, tokens, experts, part)
    own = exchanged(outgoing).reshape(experts * CAP, part)
    source = (x - jnp.arange(columns, dtype=jnp.int32)) % columns
    parts = over_columns(partial_of(source, own, wide, wide_other))
    act_all = over_columns(act_of(parts))
    val = down_of(source, act_all, down, down_other)
    back = exchanged(val.reshape(experts, CAP, part))
    return combine(back, weight)


def solution(mesh):
    return jax.shard_map(
        body,
        mesh=mesh,
        in_specs=(
            P(("groups", "expert"), None),
            P(("groups", "expert"), None),
            P(("groups", "expert"), None),
            P("expert", None, "hidden"),
            P("expert", None, "hidden"),
            P("expert", "hidden", None),
        ),
        out_specs=P(("groups", "expert"), "hidden"),
        check_vma=False,
    )
```

```python
import jax
import jax.numpy as jnp
from jax import lax
from jax.experimental import pallas as pl
from jax.experimental.pallas import tpu as pltpu
from jax.sharding import PartitionSpec as P


SPAN = 2
CAP = 8
F32 = jnp.float32
BF = jnp.bfloat16
VM = pltpu.MemorySpace.VMEM
HB = pltpu.MemorySpace.HBM


def stride(experts):
    return max(1, experts // 2 - 1)


def pack_kernel(x_ref, ids_hbm, scores_hbm, tok_hbm, out_ref, weight_ref, ids_ref, scores_ref, tok_ref, sems):
    width = tok_ref.shape[1]
    col = pl.multiple_of(x_ref[0] * width, width)
    copies = [
        pltpu.make_async_copy(ids_hbm, ids_ref, sems.at[0]),
        pltpu.make_async_copy(scores_hbm, scores_ref, sems.at[1]),
        pltpu.make_async_copy(tok_hbm.at[:, pl.ds(col, width)], tok_ref, sems.at[2]),
    ]
    for copy in copies:
        copy.start()
    for copy in copies:
        copy.wait()
    top, count = ids_ref.shape
    experts, cap, _ = out_ref.shape
    pairs = experts * cap
    scores = scores_ref[...]
    routed = 2.5 * scores / jnp.sum(scores, axis=0, keepdims=True)
    row = lax.broadcasted_iota(jnp.int32, (pairs, count), 0)
    expert = row // cap * stride(experts) % experts
    member = jnp.zeros((pairs, count), F32)
    weight = jnp.zeros((pairs, count), F32)
    for k in range(top):
        hit = ids_ref[k : k + 1, :] == expert
        member = jnp.where(hit, 1.0, member)
        weight = jnp.where(hit, routed[k : k + 1, :], weight)
    earlier = lax.broadcasted_iota(jnp.int32, (count, count), 0) < lax.broadcasted_iota(
        jnp.int32, (count, count), 1
    )
    place = jnp.dot(
        member.astype(BF), jnp.where(earlier, 1.0, 0.0).astype(BF), preferred_element_type=F32
    )
    mine = (member > 0.5) & (place == (row % cap).astype(F32))
    weight_ref[...] = jnp.where(mine, weight, 0.0)
    chosen = jnp.where(mine, 1.0, 0.0).astype(BF)
    rows = jnp.dot(chosen, tok_ref[...], preferred_element_type=F32)
    for e in range(experts):
        out_ref[e] = rows[e * cap : (e + 1) * cap].astype(BF)


def pack(x, ids, scores, tokens, experts, part):
    count = tokens.shape[0]
    return pl.pallas_call(
        pack_kernel,
        out_shape=(
            jax.ShapeDtypeStruct((experts, CAP, part), BF),
            jax.ShapeDtypeStruct((experts * CAP, count), F32),
        ),
        in_specs=[pl.BlockSpec(memory_space=pltpu.MemorySpace.SMEM)] + [pl.BlockSpec(memory_space=HB)] * 3,
        out_specs=[pl.BlockSpec(memory_space=VM)] * 2,
        scratch_shapes=[
            pltpu.VMEM(ids.shape, ids.dtype),
            pltpu.VMEM(scores.shape, scores.dtype),
            pltpu.VMEM((count, part), tokens.dtype),
            pltpu.SemaphoreType.DMA((3,)),
        ],
        name="pack",
    )(x, ids, scores, tokens)


def partial_kernel(at_ref, rows_hbm, own_ref, other_hbm, out_hbm, rows_ref, other_ref, out_ref, fetch_sems, sems, sem):
    blocks = own_ref.shape[0]
    fetches = [pltpu.make_async_copy(other_hbm.at[s], other_ref.at[s], fetch_sems.at[s]) for s in range(blocks)]
    first = pltpu.make_async_copy(rows_hbm, rows_ref, sem)
    first.start()
    for fetch in fetches:
        fetch.start()
    first.wait()
    rows = rows_ref[...]
    stores = []
    for s in range(blocks):
        fetches[s].wait()
        weights = jnp.concatenate([r[s, i] for r in (own_ref, other_ref) for i in range(2)], axis=1)
        out_ref[s] = jnp.dot(rows, weights, preferred_element_type=F32).astype(BF)
        stores.append(pltpu.make_async_copy(out_ref.at[s], out_hbm.at[at_ref[s]], sems.at[s]))
        stores[-1].start()
    for store in stores:
        store.wait()


def partial_of(at, rows, own, other):
    blocks, _, _, width = own.shape
    shape = (blocks, rows.shape[0], 2 * SPAN * width)
    return pl.pallas_call(
        partial_kernel,
        out_shape=pltpu.MemorySpace.HBM(shape, BF),
        in_specs=[
            pl.BlockSpec(memory_space=pltpu.MemorySpace.SMEM),
            pl.BlockSpec(memory_space=HB),
            pl.BlockSpec(memory_space=VM),
            pl.BlockSpec(memory_space=HB),
        ],
        out_specs=pl.BlockSpec(memory_space=HB),
        scratch_shapes=[
            pltpu.VMEM(rows.shape, BF),
            pltpu.VMEM(other.shape, BF),
            pltpu.VMEM(shape, BF),
            pltpu.SemaphoreType.DMA((blocks,)),
            pltpu.SemaphoreType.DMA((blocks,)),
            pltpu.SemaphoreType.DMA,
        ],
        compiler_params=pltpu.CompilerParams(vmem_limit_bytes=24 << 20),
        name="partial",
    )(at, pltpu.with_memory_space_constraint(rows, pltpu.MemorySpace.HBM), own, pltpu.with_memory_space_constraint(other, pltpu.MemorySpace.HBM))


def act_kernel(parts_ref, out_ref):
    blocks = parts_ref.shape[0]
    width = out_ref.shape[3]
    val = parts_ref[0].astype(F32)
    for i in range(1, blocks):
        val = val + parts_ref[i].astype(F32)
    for i in range(SPAN):
        gate = val[:, 2 * i * width : (2 * i + 1) * width]
        up = val[:, (2 * i + 1) * width : (2 * i + 2) * width]
        act = (gate / (1.0 + jnp.exp(-gate)) * up).astype(BF)
        for copy in range(blocks):
            out_ref[copy, i] = act


def act_of(parts):
    blocks, count, width = parts.shape
    return pl.pallas_call(
        act_kernel,
        out_shape=jax.ShapeDtypeStruct((blocks, SPAN, count, width // (2 * SPAN)), BF),
        in_specs=[pl.BlockSpec(memory_space=VM)],
        out_specs=pl.BlockSpec(memory_space=VM),
        compiler_params=pltpu.CompilerParams(vmem_limit_bytes=24 << 20),
        name="act",
    )(parts)


def down_kernel(at_ref, act_ref, own_ref, other_ref, out_ref):
    blocks, width, part = own_ref.shape
    val = None
    for slot, weights_ref in enumerate((own_ref, other_ref)):
        rows = jnp.concatenate([act_ref[at_ref[i], slot] for i in range(blocks)], axis=1)
        more = jnp.dot(rows, weights_ref[...].reshape(blocks * width, part), preferred_element_type=F32)
        val = more if val is None else val + more
    out_ref[...] = val.astype(BF)


def down_of(at, act, own, other):
    return pl.pallas_call(
        down_kernel,
        out_shape=jax.ShapeDtypeStruct((act.shape[2], own.shape[2]), BF),
        in_specs=[pl.BlockSpec(memory_space=pltpu.MemorySpace.SMEM)] + [pl.BlockSpec(memory_space=VM)] * 3,
        out_specs=pl.BlockSpec(memory_space=VM),
        compiler_params=pltpu.CompilerParams(vmem_limit_bytes=24 << 20),
        name="down",
    )(at, act, own, other)


def combine_kernel(back_ref, weight_ref, out_ref):
    experts = back_ref.shape[0]
    weight = weight_ref[...]
    high = weight.astype(BF)
    rest = weight - high.astype(F32)
    middle = rest.astype(BF)
    low = (rest - middle.astype(F32)).astype(BF)
    over_rows = (((0,), (0,)), ((), ()))
    rows = jnp.concatenate([back_ref[e].astype(F32) for e in range(experts)], axis=0).astype(BF)
    val = None
    for term in (low, middle, high):
        more = lax.dot_general(term, rows, over_rows, preferred_element_type=F32)
        val = more if val is None else val + more
    out_ref[...] = val.astype(BF)


def combine(back, weight):
    return pl.pallas_call(
        combine_kernel,
        out_shape=jax.ShapeDtypeStruct((weight.shape[1], back.shape[2]), BF),
        in_specs=[pl.BlockSpec(memory_space=VM)] * 2,
        out_specs=pl.BlockSpec(memory_space=VM),
        compiler_params=pltpu.CompilerParams(vmem_limit_bytes=24 << 20),
        name="combine",
    )(back, weight)


def body(tokens, expert_ids, router_scores, gate_weight, up_weight, down_weight):
    slots, columns = lax.axis_size("expert"), lax.axis_size("hidden")
    experts = slots // SPAN
    part = tokens.shape[1] // columns
    x = lax.axis_index("hidden").astype(jnp.int32)
    order = [j * stride(experts) % experts for j in range(experts)]
    same_core = [[SPAN * z + core for z in order] for core in range(SPAN)]
    swap = [(i, i ^ 1) for i in range(slots)]

    def turned(v, s):
        return lax.ppermute(v, "hidden", [(i, (i + s) % columns) for i in range(columns)])

    def swapped(v):
        return lax.ppermute(v, "expert", swap)

    def exchanged(v):
        return lax.all_to_all(
            v, "expert", split_axis=0, concat_axis=0, tiled=True, axis_index_groups=same_core
        )

    def over_columns(v):
        return lax.all_to_all(v, "hidden", split_axis=0, concat_axis=0, tiled=True)

    downs, others = [], []
    for s in range(columns):
        at = (x + s) % columns * part
        share = lax.dynamic_slice_in_dim(down_weight[0], at, part, 1)
        both = jnp.stack([lax.dynamic_slice_in_dim(w[0], at, part, 0) for w in (gate_weight, up_weight)])
        downs.append(turned(share, s) if s else share)
        others.append(turned(both, s) if s else both)
    down = jnp.stack(downs)
    wide = jnp.stack(others)
    wide_other = swapped(wide)
    down_other = swapped(down)
    outgoing, weight = pack(x.reshape(1), expert_ids.T, router_scores.T, tokens, experts, part)
    own = exchanged(outgoing).reshape(experts * CAP, part)
    source = (x - jnp.arange(columns, dtype=jnp.int32)) % columns
    parts = over_columns(partial_of(source, own, wide, wide_other))
    act_all = over_columns(act_of(parts))
    val = down_of(source, act_all, down, down_other)
    back = exchanged(val.reshape(experts, CAP, part))
    return combine(back, weight)


def solution(mesh):
    return jax.shard_map(
        body,
        mesh=mesh,
        in_specs=(
            P(("groups", "expert"), None),
            P(("groups", "expert"), None),
            P(("groups", "expert"), None),
            P("expert", None, "hidden"),
            P("expert", None, "hidden"),
            P("expert", "hidden", None),
        ),
        out_specs=P(("groups", "expert"), "hidden"),
        check_vma=False,
    )
```
